32 devices in a mesh: replica: 4 (over y, core), fsdp: 8 (over z, x).
Axes of the slice: x: 2, y: 2, z: 4, core: 2. Of those that a mesh axis runs over, the one named last changes fastest.
Arguments:
- hidden_states: bfloat16 [4, 2048, 4096], P('replica', 'fsdp'), may hold values from -6 to 6
- norm_gain: bfloat16 [4, 4096], P('replica', 'fsdp'), may hold values from 0.5 to 1.5
- key_weight: bfloat16 [4, 4096, 1024], P('replica', 'fsdp'), may hold values from -0.09375 to 0.09375
- value_weight: bfloat16 [4, 4096, 1024], P('replica', 'fsdp'), may hold values from -0.09375 to 0.09375
- deltas: float32 [4, 256, 4096], P('replica', 'fsdp'), may hold values from -6 to 6
- outer_params: float32 [256, 4096], P('fsdp', 'replica'), may hold values from -6 to 6
- momentum: float32 [256, 4096], P('fsdp', 'replica'), may hold values from -3 to 3
- local_params: bfloat16 [4, 256, 4096], P('replica', 'fsdp'), may hold values from -6 to 6
Outputs:
- keys: bfloat16 [4, 2048, 1024], P('replica', 'fsdp')
- values: bfloat16 [4, 2048, 1024], P('replica', 'fsdp')
- momentum_new: float32 [256, 4096], P('fsdp', 'replica')
- outer_new: float32 [256, 4096], P('fsdp', 'replica')
- local_new: bfloat16 [4, 256, 4096], P('replica', 'fsdp')
The draws below stay inside these ranges and needn't reach their ends.
All inputs are finite; a program needn't handle non-finite values.
Results may differ from the reference program's by a relative error of at most 0.0085.
Values may be sent and summed in bfloat16 or wider, within the bound.
A program may use at most 128 MiB of HBM per device.

```python
import jax
import jax.numpy as jnp
from jax import lax

D = 4096
HEAD = 128
KV = 1024
TOK_DEV = 256
TOKENS_R = 2048
FRAG_ROWS = 256
N_REPLICA = 4


def raised(entries, key, source, target, parts, factor):
    def block_of(axis_at):
        return (jnp.arange(entries.shape[axis_at]) // (entries.shape[axis_at] // parts)).reshape((-1,) + (1,) * (entries.ndim - 1 - axis_at))

    one_side = jax.random.permutation(key, parts)[block_of(target)]
    second = (block_of(target) + parts // 2) % parts
    return jnp.where((block_of(source) == one_side) | (block_of(source) == second), factor * entries, entries)


def levels(rng, extent, pieces, smallest, high):
    loudness = 1.0
    for position, shards_of in pieces:
        draws = jax.random.uniform(jax.random.fold_in(jax.random.fold_in(rng, 6), position), (shards_of,), jnp.float32, smallest / len(pieces), high / len(pieces))
        loudness = loudness * jnp.repeat(jnp.exp(draws), extent[position] // shards_of).reshape((-1,) + (1,) * (len(extent) - 1 - position))
    return loudness


def bell_draw(key, dims, deviation, reach, shards=(), held_as=jnp.bfloat16):
    values = deviation * jax.random.normal(key, dims, jnp.float32)
    if shards:
        values = values * levels(key, dims, shards, -0.22, 0.18)
    return jnp.clip(values, -reach, reach).astype(held_as)


def heavy_noise(stream_key, shape, scale, most, shards, heavy, kind=jnp.bfloat16):
    result = scale * jax.random.normal(stream_key, shape, jnp.float32)
    if shards:
        result = result * levels(stream_key, shape, shards, -0.22, 0.18)
    return jnp.clip(raised(result, jax.random.fold_in(stream_key, 3), *heavy), -most, most).astype(kind)


def setup_inputs(seed: int = 0) -> dict:
    key_list = jax.random.split(jax.random.key(seed), 9)
    return {
        "hidden_states": bell_draw(key_list[0], (N_REPLICA, TOKENS_R, D), 1.0, 6.0, ((0, 4), (1, 8))),
        "norm_gain": jnp.clip(1.0 + 0.1 * jax.random.normal(key_list[1], (N_REPLICA, D), jnp.float32), 0.5, 1.5).astype(jnp.bfloat16),
        "key_weight": bell_draw(key_list[2], (N_REPLICA, D, KV), D ** -0.5, 0.09375, ((0, 4), (1, 8))),
        "value_weight": bell_draw(key_list[3], (N_REPLICA, D, KV), D ** -0.5, 0.09375, ((0, 4), (1, 8))),
        "deltas": heavy_noise(key_list[4], (N_REPLICA, FRAG_ROWS, D), 1.0, 6.0, ((0, 4), (1, 8)), (0, 2, 4, 2.0), jnp.float32),
        "outer_params": bell_draw(key_list[5], (FRAG_ROWS, D), 1.0, 6.0, ((0, 8), (1, 4)), jnp.float32),
        "momentum": bell_draw(key_list[6], (FRAG_ROWS, D), 0.5, 3.0, ((0, 8), (1, 4)), jnp.float32),
        "local_params": bell_draw(key_list[7], (N_REPLICA, FRAG_ROWS, D), 1.0, 6.0, ((0, 4), (1, 8))),
    }


def rotate_keys(keys_raw, positions, head_size):
    half_width = head_size // 2
    exponent = jnp.arange(half_width, dtype=jnp.float32) * (2.0 / head_size)
    frequency = jnp.power(jnp.float32(500000.0), -exponent)
    angles = positions.astype(jnp.float32)[:, None] * frequency[None, :]
    cosine_table = jnp.cos(angles)[:, None, :]
    sine_table = jnp.sin(angles)[:, None, :]
    shaped = keys_raw.reshape(keys_raw.shape[0], -1, head_size)
    first_half = shaped[:, :, :half_width]
    second_half = shaped[:, :, half_width:]
    turned = jnp.concatenate([first_half * cosine_table - second_half * sine_table, second_half * cosine_table + first_half * sine_table], axis=2)
    return turned.reshape(keys_raw.shape)

def project_replica(inputs):
    states, gain, weight_key, weight_value = inputs
    states32 = states.astype(jnp.float32)
    inv_rms = lax.rsqrt(lax.optimization_barrier(jnp.mean(states32 * states32, axis=1, keepdims=True)) + 1e-05)
    normed = (states32 * inv_rms * gain.astype(jnp.float32)[None, :]).astype(jnp.bfloat16)
    keys_raw = jnp.dot(normed, weight_key, preferred_element_type=jnp.float32)
    values_raw = jnp.dot(normed, weight_value, preferred_element_type=jnp.float32)
    positions = jnp.arange(states.shape[0], dtype=jnp.int32) % TOK_DEV
    rotated = rotate_keys(keys_raw, positions, HEAD)
    return (rotated.astype(jnp.bfloat16), values_raw.astype(jnp.bfloat16))

def reference(hidden_states, norm_gain, key_weight, value_weight, deltas, outer_params, momentum, local_params):
    keys, values = lax.map(project_replica, (hidden_states, norm_gain, key_weight, value_weight))
    avg_delta = lax.optimization_barrier(jnp.sum(deltas, axis=0)) / deltas.shape[0]
    momentum_new = 0.9 * momentum + avg_delta
    outer_new = outer_params - 0.7 * (avg_delta + 0.9 * momentum_new)
    local_new = (0.5 * local_params.astype(jnp.float32) + 0.5 * outer_new[None, :, :]).astype(jnp.bfloat16)
    return (keys, values, momentum_new, outer_new, local_new)
```

```python
import functools

import jax
import jax.numpy as jnp
import numpy as np
from jax import lax
from jax.experimental import pallas as pl
from jax.experimental.pallas import tpu as pltpu
from jax.sharding import PartitionSpec as P

HEAD = 128
MESH = pl.DeviceIdType.MESH


def rotation_tables(tokens, head_size):
    half_width = head_size // 2
    exponent = np.arange(half_width, dtype=np.float32) * np.float32(2.0 / head_size)
    frequency = np.power(np.float32(500000.0), -exponent)
    angles = np.arange(tokens, dtype=np.float32)[:, None] * frequency[None, :]
    cosine, sine = np.cos(angles), np.sin(angles)
    return (
        jnp.asarray(np.concatenate([cosine, cosine], axis=1)),
        jnp.asarray(np.concatenate([-sine, sine], axis=1)),
    )


def write_out(*refs):
    count = len(refs) // 2
    sems = refs[-1]
    copies = [
        pltpu.make_async_copy(refs[i], refs[count + i], sems.at[i]) for i in range(count)
    ]
    for copy in copies:
        copy.start()
    for copy in copies:
        copy.wait()


def kernel(
    groups, replicas, width,
    hs, gain, kw, vw, cosine_in, sine_in, deltas, outer_in, momentum_in, local_in,
    keys_out, values_out, momentum_out, outer_out, local_out,
    cosine, sine, deltas_own, outer, momentum, local,
    keys, values, momentum_new, outer_new, local_new,
    hs_v, gains, a_in, a_scaled, a_own, weights, inv, acc, c_out, c_in, d_in, o_in,
    hs_sem, g_sem, a_sem, own_sem, w_recv, x_send, z_send, f_send, e_send,
    c_send, c_recv, d_sem, o_sem, load_sem, store_sem,
):
    h = groups // 2
    r, f = lax.axis_index("replica"), lax.axis_index("fsdp")
    x, g = lax.rem(f, 2), lax.div(f, 2)
    half = lax.div(g, h)
    local_g = lax.rem(g, h)
    d = (h - 1 - local_g) * (1 - half) + local_g * half
    tokens, depth = hs.shape[0], kw.shape[0]
    half_depth = 2 * h * depth
    per_weight = kw.shape[1] // width
    chunks = 2 * per_weight
    first = chunks // 2
    split = chunks - chunks // 4
    early = chunks // 4
    own_w = outer.shape[1]
    features = hs.shape[1]

    def place(dist):
        return (h - 1 - dist) * (1 - half) + dist * half

    def slot(dist, side):
        return 2 * place(dist) + side

    def device(dist, side):
        return {"fsdp": 2 * (half * h + place(dist)) + side}

    def other_half(dist):
        return {"fsdp": 2 * ((1 - half) * (h + dist) + half * (h - 1 - dist)) + x}

    partner = device(d, 1 - x)
    outer_peers = [(0, True)] + [(1 + lax.rem(d - 1 + j, h - 1), False) for j in range(1, h - 1)]
    inner_peers = [(j, False) for j in range(1, h)]
    is_inner = d == 0

    def replica_at(j):
        return lax.rem(r + j, replicas)

    def mates():
        me = 2 * local_g + x
        return [
            {"fsdp": half * 2 * h + lax.rem(me + j, 2 * h)} for j in range(1, 2 * h)
        ]

    barrier = pltpu.get_barrier_semaphore()

    def greet(target):
        pl.semaphore_signal(barrier, inc=1, device_id=target, device_id_type=MESH)

    for target in mates():
        greet(target)
    greet(other_half(0))
    for j in range(1, replicas):
        greet({"replica": replica_at(j)})

    @pl.when(is_inner)
    def _():
        for i in range(h):
            greet(other_half(i))

    def remote(src, dst, send, recv, target):
        return pltpu.make_async_remote_copy(
            src_ref=src, dst_ref=dst, send_sem=send, recv_sem=recv,
            device_id=target, device_id_type=MESH,
        )

    mine = pl.ds(pl.multiple_of(r * own_w, own_w), own_w)
    hs_copy = pltpu.make_async_copy(hs, hs_v, hs_sem)
    hs_copy.start()
    my_slot = slot(d, x)
    partner_slot = slot(d, 1 - x)

    def rows(q):
        return pl.ds(pl.multiple_of(q * depth, depth), depth)

    def source(c):
        return (kw if c < per_weight else vw).at[:, pl.ds((c % per_weight) * width, width)]

    own_copies = []
    for c in range(chunks):
        own_copies.append(
            pltpu.make_async_copy(source(c), weights.at[c, rows(my_slot)], own_sem.at[c])
        )
        own_copies[-1].start()
    loads = [
        pltpu.make_async_copy(src, dst, load_sem.at[i])
        for i, (src, dst) in enumerate(
            (
                (deltas.at[:, mine], deltas_own),
                (outer_in, outer),
                (momentum_in, momentum),
                (local_in, local),
                (cosine_in, cosine),
                (sine_in, sine),
            )
        )
    ]

    pl.semaphore_wait(
        barrier, (2 * h - 1) + 1 + (replicas - 1) + jnp.where(is_inner, h, 0)
    )

    def x_copy(c):
        return remote(
            source(c), weights.at[c, rows(my_slot)], x_send.at[c], w_recv.at[c, my_slot], partner
        )

    def z_copy(c, j, dist):
        return remote(
            source(c), weights.at[c, rows(my_slot)], z_send.at[j, c], w_recv.at[c, my_slot],
            device(dist, x),
        )

    def f_copy(c, j, dist):
        q = slot(dist, x)
        return remote(
            weights.at[c, rows(q)], weights.at[c, rows(q)], f_send.at[j, c], w_recv.at[c, q],
            partner,
        )

    def e_copy(c, j, dist):
        return remote(
            weights.at[c, rows(partner_slot)], weights.at[c, rows(partner_slot)],
            e_send.at[j, c], w_recv.at[c, partner_slot], device(dist, x),
        )

    def arrived(c, q):
        remote(
            kw.at[:, pl.ds(0, width)], weights.at[c, rows(q)], x_send.at[0], w_recv.at[c, q],
            partner,
        ).wait_recv()

    away = pl.ds(pl.multiple_of((1 - half) * half_depth, half_depth), half_depth)
    a_copy = remote(hs.at[:, away], a_in.at[d], a_sem.at[0], a_sem.at[1 + d], other_half(0))

    @pl.when(is_inner)
    def _():
        for c in range(2):
            x_copy(c).start()
        a_copy.start()
        for c in range(chunks):
            for j, (dist, _) in enumerate(inner_peers):
                z_copy(c, j, dist).start()

    @pl.when(jnp.logical_not(is_inner))
    def _():
        for c in range(chunks):
            if c == first:
                a_copy.start()
            for j, (dist, _) in enumerate(outer_peers):
                z_copy(c, j, dist).start()
        for c in list(range(split, chunks)) + list(range(early)):
            x_copy(c).start()

    g_copies = []
    for j, target in enumerate(mates()):
        g_copies.append(
            remote(gain, gains.at[my_slot], g_sem.at[j], g_sem.at[2 * h - 1 + my_slot], target)
        )
        g_copies[-1].start()
    d_copies = []
    for j in range(1, replicas):
        columns = pl.ds(pl.multiple_of(replica_at(j) * own_w, own_w), own_w)
        d_copies.append(
            remote(
                deltas.at[:, columns], d_in.at[j - 1], d_sem.at[0, j - 1], d_sem.at[1, j - 1],
                {"replica": replica_at(j)},
            )
        )
        d_copies[-1].start()
    for copy in loads:
        copy.start()

    hs_copy.wait()
    total = jnp.zeros((tokens, 1), jnp.float32)
    part_w = 2 * depth
    for k in range(features // part_w):
        part = hs_v[:, k * part_w : (k + 1) * part_w].astype(jnp.float32)
        total += jnp.sum(part * part, axis=1, keepdims=True)
    inv[...] = jnp.broadcast_to(lax.rsqrt(total / features + 1e-05), inv.shape)

    gains[my_slot] = gain[...]
    for j in range(1, 2 * h):
        q = lax.rem(my_slot + j, 2 * h)
        remote(gain, gains.at[q], g_sem.at[0], g_sem.at[2 * h - 1 + q], partner).wait_recv()

    def scale(target, origin, base):
        for q in range(2 * h):
            at = pl.ds(base + q * depth, depth)
            target[:, q * depth : (q + 1) * depth] = (
                origin[:, at].astype(jnp.float32) * gains[q].astype(jnp.float32)
            ).astype(jnp.bfloat16)

    @pl.when(half == 0)
    def _():
        scale(a_own, hs_v, 0)

    @pl.when(half == 1)
    def _():
        scale(a_own, hs_v, half_depth)

    def own_product(c):
        acc[c] = jnp.dot(a_own[...], weights[c], preferred_element_type=jnp.float32)

    def back_copy(i, c):
        return remote(c_out.at[i, c], c_in.at[c], c_send.at[i, c], c_recv.at[c], other_half(i))

    def away_product(i, c):
        c_out[i, c] = jnp.dot(
            a_scaled[i], weights[c], preferred_element_type=jnp.float32
        ).astype(jnp.bfloat16)
        back_copy(i, c).start()

    def own_wait(c):
        pltpu.make_async_copy(
            kw.at[:, pl.ds(0, width)], weights.at[c, rows(my_slot)], own_sem.at[c]
        ).wait()

    def outer_step():
        for copy in loads:
            copy.wait()
        avg = deltas_own[...]
        for j in range(1, replicas):
            d_copies[j - 1].wait_recv()
            avg += d_in[j - 1]
        avg = avg / replicas
        moved = 0.9 * momentum[...] + avg
        momentum_new[...] = moved
        outer_new[...] = outer[...] - 0.7 * (avg + 0.9 * moved)
        store(0, momentum_new, momentum_out).start()
        store(1, outer_new, outer_out).start()
        for j in range(1, replicas):
            o_copy(j).start()

    def merge_step():
        part = jnp.float32(0.5)
        local_new[:, mine] = (
            part * local[:, mine].astype(jnp.float32) + part * outer_new[...]
        ).astype(jnp.bfloat16)
        for j in range(1, replicas):
            o_copy(j).wait_recv()
            theirs = pl.ds(
                pl.multiple_of(lax.rem(r + replicas - j, replicas) * own_w, own_w), own_w
            )
            local_new[:, theirs] = (
                part * local[:, theirs].astype(jnp.float32) + part * o_in[j - 1]
            ).astype(jnp.bfloat16)
        store(2, local_new, local_out).start()

    def o_copy(j):
        return remote(
            outer_new, o_in.at[j - 1], o_sem.at[0, j - 1], o_sem.at[1, j - 1],
            {"replica": replica_at(j)},
        )

    def store(i, src, dst):
        return pltpu.make_async_copy(src, dst, store_sem.at[i])

    def result_copy(src, dst, c, sem):
        at = pl.ds(pl.multiple_of(c * width, width), width)
        return pltpu.make_async_copy(src.at[:, at], dst.at[:, at], store_sem.at[sem])

    @pl.when(is_inner)
    def _():
        def pass_on(c):
            for j, (dist, _) in enumerate(inner_peers):
                arrived(c, slot(dist, x))
                if c < split:
                    f_copy(c, j, dist).start()

        for c in range(first):
            pass_on(c)
            if c + 2 < first:
                x_copy(c + 2).start()
            if c < early:
                arrived(c, partner_slot)
                for j, (dist, _) in enumerate(inner_peers):
                    e_copy(c, j, dist).start()
            if c == 0:
                outer_step()
            if c == 1:
                merge_step()
        for c in range(first, split):
            x_copy(c).start()

        def rest(c, known):
            own_wait(c)
            if not known:
                arrived(c, partner_slot)
            for dist, _ in inner_peers:
                arrived(c, slot(dist, 1 - x))

        remote(hs.at[:, away], a_in.at[0], a_sem.at[0], a_sem.at[1], partner).wait_recv()
        for q in range(2 * h):
            at = slice(q * depth, (q + 1) * depth)
            a_scaled[0, :, at] = (
                a_in[0, :, at].astype(jnp.float32) * gains[q].astype(jnp.float32)
            ).astype(jnp.bfloat16)

        @pl.loop(0, early)
        def _(c):
            rest(c, True)
            away_product(0, c)
            own_product(c)

        @pl.loop(early, first)
        def _(c):
            rest(c, False)
            away_product(0, c)
            own_product(c)

        for i in range(1, h):
            remote(
                hs.at[:, away], a_in.at[i], a_sem.at[0], a_sem.at[1 + i], partner
            ).wait_recv()
            for q in range(2 * h):
                at = slice(q * depth, (q + 1) * depth)
                a_scaled[i, :, at] = (
                    a_in[i, :, at].astype(jnp.float32) * gains[q].astype(jnp.float32)
                ).astype(jnp.bfloat16)

            @pl.loop(0, first)
            def _(c):
                away_product(i, c)

        pass_on(first)
        for c in range(first, chunks):
            if c + 1 < chunks:
                pass_on(c + 1)
            if c + 1 == split - 1:
                for k in range(split, chunks):
                    x_copy(k).start()
            rest(c, False)
            for i in range(h):
                away_product(i, c)
            own_product(c)

    @pl.when(jnp.logical_not(is_inner))
    def _():
        for c in range(chunks):
            for j, (dist, _) in enumerate(outer_peers):
                arrived(c, slot(dist, x))
                if c >= early:
                    f_copy(c, j, dist).start()
            if early <= c < split:
                x_copy(c).start()
            if c == 1:
                for k in range(split, chunks):
                    arrived(k, partner_slot)
                    for j, (dist, inner) in enumerate(outer_peers):
                        if inner:
                            e_copy(k, j, dist).start()
                outer_step()
            if c == 2:
                for k in range(early):
                    arrived(k, partner_slot)
                    for j, (dist, inner) in enumerate(outer_peers):
                        if not inner:
                            e_copy(k, j, dist).start()
                merge_step()

        def finish(c, known):
            own_wait(c)
            if not known:
                arrived(c, partner_slot)
            for dist, _ in outer_peers:
                arrived(c, slot(dist, 1 - x))
            own_product(c)

        @pl.loop(early, split)
        def _(c):
            finish(c, False)

        @pl.loop(0, early)
        def _(c):
            finish(c, True)

        @pl.loop(split, chunks)
        def _(c):
            finish(c, True)

    def summed(c):
        back_copy(0, c).wait_recv()
        return (acc[c] + c_in[c].astype(jnp.float32)) * inv[:, 0:1]

    @pl.loop(0, per_weight)
    def _(c):
        value = summed(c)
        for k in range(width // HEAD):
            head = value[:, k * HEAD : (k + 1) * HEAD]
            turned = head * cosine[...] + pltpu.roll(head, HEAD // 2, 1) * sine[...]
            at = pl.ds(pl.multiple_of(c * width + k * HEAD, HEAD), HEAD)
            keys[:, at] = turned.astype(jnp.bfloat16)
        result_copy(keys, keys_out, c, 3 + c).start()

    @pl.loop(0, per_weight)
    def _(c):
        at = pl.ds(pl.multiple_of(c * width, width), width)
        values[:, at] = summed(c + per_weight).astype(jnp.bfloat16)
        result_copy(values, values_out, c, 3 + per_weight + c).start()

    a_copy.wait_send()
    for copy in g_copies + d_copies:
        copy.wait_send()
    for j in range(1, replicas):
        o_copy(j).wait_send()

    @pl.loop(0, chunks)
    def _(c):
        remote(
            kw.at[:, pl.ds(0, width)], weights.at[c, rows(my_slot)], x_send.at[c],
            w_recv.at[c, my_slot], partner,
        ).wait_send()
        for j in range(h - 1):
            remote(
                kw.at[:, pl.ds(0, width)], weights.at[c, rows(my_slot)], z_send.at[j, c],
                w_recv.at[c, my_slot], partner,
            ).wait_send()

    @pl.when(is_inner)
    def _():
        @pl.loop(0, chunks)
        def _(c):
            for i in range(h):
                back_copy(i, c).wait_send()

        for j, (dist, _) in enumerate(inner_peers):
            for c in range(split):
                f_copy(c, j, dist).wait_send()
            for c in range(early):
                e_copy(c, j, dist).wait_send()

    @pl.when(jnp.logical_not(is_inner))
    def _():
        for j, (dist, inner) in enumerate(outer_peers):
            for c in range(early, chunks):
                f_copy(c, j, dist).wait_send()
            for c in range(split, chunks) if inner else range(early):
                e_copy(c, j, dist).wait_send()

    store(0, momentum_new, momentum_out).wait()
    store(1, outer_new, outer_out).wait()
    store(2, local_new, local_out).wait()

    @pl.loop(0, per_weight)
    def _(c):
        result_copy(keys, keys_out, c, 3 + c).wait()
        result_copy(values, values_out, c, 3 + per_weight + c).wait()


def per_device(
    groups, replicas,
    hidden_states, norm_gain, key_weight, value_weight, deltas, outer_params, momentum, local_params,
):
    hs, kw, vw = hidden_states[0], key_weight[0], value_weight[0]
    tokens, features = hs.shape
    depth, kv = kw.shape
    width = 2 * HEAD
    chunks = 2 * kv // width
    h = groups // 2
    half_depth = groups * depth
    cosine, sine = rotation_tables(tokens, HEAD)
    own = outer_params.shape
    vmem = pl.BlockSpec(memory_space=pltpu.VMEM)
    hbm = pl.BlockSpec(memory_space=pl.ANY)
    dma = pltpu.SemaphoreType.DMA
    bf16, f32 = jnp.bfloat16, jnp.float32
    results = pl.pallas_call(
        functools.partial(kernel, groups, replicas, width),
        out_shape=(
            jax.ShapeDtypeStruct((tokens, kv), bf16),
            jax.ShapeDtypeStruct((tokens, kv), bf16),
            jax.ShapeDtypeStruct(own, f32),
            jax.ShapeDtypeStruct(own, f32),
            jax.ShapeDtypeStruct(local_params.shape[1:], bf16),
        ),
        in_specs=[hbm, vmem] + [hbm] * 8,
        out_specs=[hbm] * 5,
        scratch_shapes=[
            pltpu.VMEM(cosine.shape, f32),
            pltpu.VMEM(sine.shape, f32),
            pltpu.VMEM(own, f32),
            pltpu.VMEM(own, f32),
            pltpu.VMEM(own, f32),
            pltpu.VMEM(local_params.shape[1:], bf16),
            pltpu.VMEM((tokens, kv), bf16),
            pltpu.VMEM((tokens, kv), bf16),
            pltpu.VMEM(own, f32),
            pltpu.VMEM(own, f32),
            pltpu.VMEM(local_params.shape[1:], bf16),
            pltpu.VMEM((tokens, features), bf16),
            pltpu.VMEM((2 * h, 1, depth), bf16),
            pltpu.VMEM((h, tokens, half_depth), bf16),
            pltpu.VMEM((h, tokens, half_depth), bf16),
            pltpu.VMEM((tokens, half_depth), bf16),
            pltpu.VMEM((chunks, half_depth, width), bf16),
            pltpu.VMEM((tokens, HEAD), f32),
            pltpu.VMEM((chunks, tokens, width), f32),
            pltpu.VMEM((h, chunks, tokens, width), bf16),
            pltpu.VMEM((chunks, tokens, width), bf16),
            pltpu.VMEM((replicas - 1,) + own, f32),
            pltpu.VMEM((replicas - 1,) + own, f32),
            dma,
            dma((4 * h - 1,)),
            dma((1 + h,)),
            dma((chunks,)),
            dma((chunks, 2 * h)),
            dma((chunks,)),
            dma((h - 1, chunks)),
            dma((h - 1, chunks)),
            dma((h - 1, chunks)),
            dma((h, chunks)),
            dma((chunks,)),
            dma((2, replicas - 1)),
            dma((2, replicas - 1)),
            dma((6,)),
            dma((3 + chunks,)),
        ],
        compiler_params=pltpu.CompilerParams(
            collective_id=0, has_side_effects=True, vmem_limit_bytes=60 * 1024 * 1024
        ),
    )(
        hs, norm_gain, kw, vw, cosine, sine,
        deltas[0], outer_params, momentum, local_params[0],
    )
    keys, values, momentum_new, outer_new, local_new = pl.pallas_call(
        write_out,
        out_shape=tuple(jax.ShapeDtypeStruct(a.shape, a.dtype) for a in results),
        in_specs=[vmem] * 5,
        out_specs=[hbm] * 5,
        scratch_shapes=[dma((5,))],
        compiler_params=pltpu.CompilerParams(vmem_limit_bytes=60 * 1024 * 1024),
    )(*results)
    return keys[None], values[None], momentum_new, outer_new, local_new[None]


def solution(mesh):
    in_specs = (
        P("replica", "fsdp", None),
        P("replica", "fsdp"),
        P("replica", "fsdp", None),
        P("replica", "fsdp", None),
        P("replica", "fsdp", None),
        P("fsdp", "replica"),
        P("fsdp", "replica"),
        P("replica", "fsdp", None),
    )
    out_specs = (
        P("replica", "fsdp", None),
        P("replica", "fsdp", None),
        P("fsdp", "replica"),
        P("fsdp", "replica"),
        P("replica", "fsdp", None),
    )
    groups, replicas = mesh.shape["fsdp"] // 2, mesh.shape["replica"]
    return jax.shard_map(
        functools.partial(per_device, groups, replicas),
        mesh=mesh, in_specs=in_specs, out_specs=out_specs, check_vma=False,
    )
```

```python
import functools

import jax
import jax.numpy as jnp
import numpy as np
from jax import lax
from jax.experimental import pallas as pl
from jax.experimental.pallas import tpu as pltpu
from jax.sharding import PartitionSpec as P

HEAD = 128
MESH = pl.DeviceIdType.MESH


def rotation_tables(tokens, head_size):
    half_width = head_size // 2
    exponent = np.arange(half_width, dtype=np.float32) * np.float32(2.0 / head_size)
    frequency = np.power(np.float32(500000.0), -exponent)
    angles = np.arange(tokens, dtype=np.float32)[:, None] * frequency[None, :]
    cosine, sine = np.cos(angles), np.sin(angles)
    return (
        jnp.asarray(np.concatenate([cosine, cosine], axis=1)),
        jnp.asarray(np.concatenate([-sine, sine], axis=1)),
    )


def write_out(*refs):
    count = len(refs) // 2
    sems = refs[-1]
    copies = [
        pltpu.make_async_copy(refs[i], refs[count + i], sems.at[i]) for i in range(count)
    ]
    for copy in copies:
        copy.start()
    for copy in copies:
        copy.wait()


def kernel(
    groups, replicas, width,
    hs, gain, kw, vw, cosine_in, sine_in, deltas, outer_in, momentum_in, local_in,
    keys_out, values_out, momentum_out, outer_out, local_out,
    cosine, sine, deltas_own, outer, momentum, local,
    keys, values, momentum_new, outer_new, local_new,
    hs_v, gains, a_in, a_scaled, a_own, weights, inv, acc, c_out, c_in, d_in, o_in,
    hs_sem, g_sem, a_sem, own_sem, w_recv, x_send, z_send, f_send, e_send,
    c_send, c_recv, d_sem, o_sem, load_sem, store_sem,
):
    h = groups // 2
    r, f = lax.axis_index("replica"), lax.axis_index("fsdp")
    x, g = lax.rem(f, 2), lax.div(f, 2)
    half = lax.div(g, h)
    local_g = lax.rem(g, h)
    d = (h - 1 - local_g) * (1 - half) + local_g * half
    tokens, depth = hs.shape[0], kw.shape[0]
    half_depth = 2 * h * depth
    per_weight = kw.shape[1] // width
    chunks = 2 * per_weight
    first = chunks // 2
    split = chunks - chunks // 4
    early = chunks // 4
    own_w = outer.shape[1]
    features = hs.shape[1]

    def place(dist):
        return (h - 1 - dist) * (1 - half) + dist * half

    def slot(dist, side):
        return 2 * place(dist) + side

    def device(dist, side):
        return {"fsdp": 2 * (half * h + place(dist)) + side}

    def other_half(dist):
        return {"fsdp": 2 * ((1 - half) * (h + dist) + half * (h - 1 - dist)) + x}

    partner = device(d, 1 - x)
    outer_peers = [(0, True)] + [(1 + lax.rem(d - 1 + j, h - 1), False) for j in range(1, h - 1)]
    inner_peers = [(j, False) for j in range(1, h)]
    is_inner = d == 0

    def replica_at(j):
        return lax.rem(r + j, replicas)

    def mates():
        me = 2 * local_g + x
        return [
            {"fsdp": half * 2 * h + lax.rem(me + j, 2 * h)} for j in range(1, 2 * h)
        ]

    barrier = pltpu.get_barrier_semaphore()

    def greet(target):
        pl.semaphore_signal(barrier, inc=1, device_id=target, device_id_type=MESH)

    for target in mates():
        greet(target)
    greet(other_half(0))
    for j in range(1, replicas):
        greet({"replica": replica_at(j)})

    @pl.when(is_inner)
    def _():
        for i in range(h):
            greet(other_half(i))

    def remote(src, dst, send, recv, target):
        return pltpu.make_async_remote_copy(
            src_ref=src, dst_ref=dst, send_sem=send, recv_sem=recv,
            device_id=target, device_id_type=MESH,
        )

    mine = pl.ds(pl.multiple_of(r * own_w, own_w), own_w)
    hs_copy = pltpu.make_async_copy(hs, hs_v, hs_sem)
    hs_copy.start()
    my_slot = slot(d, x)
    partner_slot = slot(d, 1 - x)

    def rows(q):
        return pl.ds(pl.multiple_of(q * depth, depth), depth)

    def source(c):
        return (kw if c < per_weight else vw).at[:, pl.ds((c % per_weight) * width, width)]

    own_copies = []
    for c in range(chunks):
        own_copies.append(
            pltpu.make_async_copy(source(c), weights.at[c, rows(my_slot)], own_sem.at[c])
        )
        own_copies[-1].start()
    loads = [
        pltpu.make_async_copy(src, dst, load_sem.at[i])
        for i, (src, dst) in enumerate(
            (
                (deltas.at[:, mine], deltas_own),
                (outer_in, outer),
                (momentum_in, momentum),
                (local_in, local),
                (cosine_in, cosine),
                (sine_in, sine),
            )
        )
    ]

    pl.semaphore_wait(
        barrier, (2 * h - 1) + 1 + (replicas - 1) + jnp.where(is_inner, h, 0)
    )

    def x_copy(c):
        return remote(
            source(c), weights.at[c, rows(my_slot)], x_send.at[c], w_recv.at[c, my_slot], partner
        )

    def z_copy(c, j, dist):
        return remote(
            source(c), weights.at[c, rows(my_slot)], z_send.at[j, c], w_recv.at[c, my_slot],
            device(dist, x),
        )

    def f_copy(c, j, dist):
        q = slot(dist, x)
        return remote(
            weights.at[c, rows(q)], weights.at[c, rows(q)], f_send.at[j, c], w_recv.at[c, q],
            partner,
        )

    def e_copy(c, j, dist):
        return remote(
            weights.at[c, rows(partner_slot)], weights.at[c, rows(partner_slot)],
            e_send.at[j, c], w_recv.at[c, partner_slot], device(dist, x),
        )

    def arrived(c, q):
        remote(
            kw.at[:, pl.ds(0, width)], weights.at[c, rows(q)], x_send.at[0], w_recv.at[c, q],
            partner,
        ).wait_recv()

    g_copies = []
    for j, target in enumerate(mates()):
        g_copies.append(
            remote(gain, gains.at[my_slot], g_sem.at[j], g_sem.at[2 * h - 1 + my_slot], target)
        )
        g_copies[-1].start()

    away = pl.ds(pl.multiple_of((1 - half) * half_depth, half_depth), half_depth)
    a_copy = remote(hs.at[:, away], a_in.at[d], a_sem.at[0], a_sem.at[1 + d], other_half(0))

    @pl.when(is_inner)
    def _():
        for c in range(2):
            x_copy(c).start()
        a_copy.start()
        for c in range(chunks):
            for j, (dist, _) in enumerate(inner_peers):
                z_copy(c, j, dist).start()

    @pl.when(jnp.logical_not(is_inner))
    def _():
        for c in range(chunks):
            if c == first:
                a_copy.start()
            for j, (dist, _) in enumerate(outer_peers):
                z_copy(c, j, dist).start()
        for c in list(range(split, chunks)) + list(range(early)):
            x_copy(c).start()

    d_copies = []
    for j in range(1, replicas):
        columns = pl.ds(pl.multiple_of(replica_at(j) * own_w, own_w), own_w)
        d_copies.append(
            remote(
                deltas.at[:, columns], d_in.at[j - 1], d_sem.at[0, j - 1], d_sem.at[1, j - 1],
                {"replica": replica_at(j)},
            )
        )
        d_copies[-1].start()
    for copy in loads:
        copy.start()

    hs_copy.wait()
    total = jnp.zeros((tokens, 1), jnp.float32)
    part_w = 2 * depth
    for k in range(features // part_w):
        part = hs_v[:, k * part_w : (k + 1) * part_w].astype(jnp.float32)
        total += jnp.sum(part * part, axis=1, keepdims=True)
    inv[...] = jnp.broadcast_to(lax.rsqrt(total / features + 1e-05), inv.shape)

    gains[my_slot] = gain[...]
    for j in range(1, 2 * h):
        q = lax.rem(my_slot + j, 2 * h)
        remote(gain, gains.at[q], g_sem.at[0], g_sem.at[2 * h - 1 + q], partner).wait_recv()

    def scale(target, origin, base):
        for q in range(2 * h):
            at = pl.ds(base + q * depth, depth)
            target[:, q * depth : (q + 1) * depth] = (
                origin[:, at].astype(jnp.float32) * gains[q].astype(jnp.float32)
            ).astype(jnp.bfloat16)

    @pl.when(half == 0)
    def _():
        scale(a_own, hs_v, 0)

    @pl.when(half == 1)
    def _():
        scale(a_own, hs_v, half_depth)

    def own_product(c):
        acc[c] = jnp.dot(a_own[...], weights[c], preferred_element_type=jnp.float32)

    def back_copy(i, c):
        return remote(c_out.at[i, c], c_in.at[c], c_send.at[i, c], c_recv.at[c], other_half(i))

    def away_product(i, c):
        c_out[i, c] = jnp.dot(
            a_scaled[i], weights[c], preferred_element_type=jnp.float32
        ).astype(jnp.bfloat16)
        back_copy(i, c).start()

    def own_wait(c):
        pltpu.make_async_copy(
            kw.at[:, pl.ds(0, width)], weights.at[c, rows(my_slot)], own_sem.at[c]
        ).wait()

    def outer_step():
        for copy in loads:
            copy.wait()
        avg = deltas_own[...]
        for j in range(1, replicas):
            d_copies[j - 1].wait_recv()
            avg += d_in[j - 1]
        avg = avg / replicas
        moved = 0.9 * momentum[...] + avg
        momentum_new[...] = moved
        outer_new[...] = outer[...] - 0.7 * (avg + 0.9 * moved)
        store(0, momentum_new, momentum_out).start()
        store(1, outer_new, outer_out).start()
        for j in range(1, replicas):
            o_copy(j).start()

    def merge_step():
        part = jnp.float32(0.5)
        local_new[:, mine] = (
            part * local[:, mine].astype(jnp.float32) + part * outer_new[...]
        ).astype(jnp.bfloat16)
        for j in range(1, replicas):
            o_copy(j).wait_recv()
            theirs = pl.ds(
                pl.multiple_of(lax.rem(r + replicas - j, replicas) * own_w, own_w), own_w
            )
            local_new[:, theirs] = (
                part * local[:, theirs].astype(jnp.float32) + part * o_in[j - 1]
            ).astype(jnp.bfloat16)
        store(2, local_new, local_out).start()

    def o_copy(j):
        return remote(
            outer_new, o_in.at[j - 1], o_sem.at[0, j - 1], o_sem.at[1, j - 1],
            {"replica": replica_at(j)},
        )

    def store(i, src, dst):
        return pltpu.make_async_copy(src, dst, store_sem.at[i])

    def result_copy(src, dst, c, sem):
        at = pl.ds(pl.multiple_of(c * width, width), width)
        return pltpu.make_async_copy(src.at[:, at], dst.at[:, at], store_sem.at[sem])

    @pl.when(is_inner)
    def _():
        def pass_on(c):
            for j, (dist, _) in enumerate(inner_peers):
                arrived(c, slot(dist, x))
                if c < split:
                    f_copy(c, j, dist).start()

        for c in range(first):
            pass_on(c)
            if c + 2 < first:
                x_copy(c + 2).start()
            if c < early:
                arrived(c, partner_slot)
                for j, (dist, _) in enumerate(inner_peers):
                    e_copy(c, j, dist).start()
            if c == 0:
                outer_step()
            if c == 1:
                merge_step()
        for c in range(first, split):
            x_copy(c).start()

        def rest(c, known):
            own_wait(c)
            if not known:
                arrived(c, partner_slot)
            for dist, _ in inner_peers:
                arrived(c, slot(dist, 1 - x))

        remote(hs.at[:, away], a_in.at[0], a_sem.at[0], a_sem.at[1], partner).wait_recv()
        for q in range(2 * h):
            at = slice(q * depth, (q + 1) * depth)
            a_scaled[0, :, at] = (
                a_in[0, :, at].astype(jnp.float32) * gains[q].astype(jnp.float32)
            ).astype(jnp.bfloat16)

        @pl.loop(0, early)
        def _(c):
            rest(c, True)
            away_product(0, c)
            own_product(c)

        @pl.loop(early, first)
        def _(c):
            rest(c, False)
            away_product(0, c)
            own_product(c)

        for i in range(1, h):
            remote(
                hs.at[:, away], a_in.at[i], a_sem.at[0], a_sem.at[1 + i], partner
            ).wait_recv()
            for q in range(2 * h):
                at = slice(q * depth, (q + 1) * depth)
                a_scaled[i, :, at] = (
                    a_in[i, :, at].astype(jnp.float32) * gains[q].astype(jnp.float32)
                ).astype(jnp.bfloat16)

            @pl.loop(0, first)
            def _(c):
                away_product(i, c)

        pass_on(first)
        for c in range(first, chunks):
            if c + 1 < chunks:
                pass_on(c + 1)
            if c + 1 == split - 1:
                for k in range(split, chunks):
                    x_copy(k).start()
            rest(c, False)
            for i in range(h):
                away_product(i, c)
            own_product(c)

    @pl.when(jnp.logical_not(is_inner))
    def _():
        for c in range(chunks):
            for j, (dist, _) in enumerate(outer_peers):
                arrived(c, slot(dist, x))
                if c >= early:
                    f_copy(c, j, dist).start()
            if early <= c < split:
                x_copy(c).start()
            if c == 1:
                for k in range(split, chunks):
                    arrived(k, partner_slot)
                    for j, (dist, inner) in enumerate(outer_peers):
                        if inner:
                            e_copy(k, j, dist).start()
                outer_step()
            if c == 2:
                for k in range(early):
                    arrived(k, partner_slot)
                    for j, (dist, inner) in enumerate(outer_peers):
                        if not inner:
                            e_copy(k, j, dist).start()
                merge_step()

        def finish(c, known):
            own_wait(c)
            if not known:
                arrived(c, partner_slot)
            for dist, _ in outer_peers:
                arrived(c, slot(dist, 1 - x))
            own_product(c)

        @pl.loop(early, split)
        def _(c):
            finish(c, False)

        @pl.loop(0, early)
        def _(c):
            finish(c, True)

        @pl.loop(split, chunks)
        def _(c):
            finish(c, True)

    def summed(c):
        back_copy(0, c).wait_recv()
        return (acc[c] + c_in[c].astype(jnp.float32)) * inv[:, 0:1]

    @pl.loop(0, per_weight)
    def _(c):
        value = summed(c)
        for k in range(width // HEAD):
            head = value[:, k * HEAD : (k + 1) * HEAD]
            turned = head * cosine[...] + pltpu.roll(head, HEAD // 2, 1) * sine[...]
            at = pl.ds(pl.multiple_of(c * width + k * HEAD, HEAD), HEAD)
            keys[:, at] = turned.astype(jnp.bfloat16)
        result_copy(keys, keys_out, c, 3 + c).start()

    @pl.loop(0, per_weight)
    def _(c):
        at = pl.ds(pl.multiple_of(c * width, width), width)
        values[:, at] = summed(c + per_weight).astype(jnp.bfloat16)
        result_copy(values, values_out, c, 3 + per_weight + c).start()

    a_copy.wait_send()
    for copy in g_copies + d_copies:
        copy.wait_send()
    for j in range(1, replicas):
        o_copy(j).wait_send()

    @pl.loop(0, chunks)
    def _(c):
        remote(
            kw.at[:, pl.ds(0, width)], weights.at[c, rows(my_slot)], x_send.at[c],
            w_recv.at[c, my_slot], partner,
        ).wait_send()
        for j in range(h - 1):
            remote(
                kw.at[:, pl.ds(0, width)], weights.at[c, rows(my_slot)], z_send.at[j, c],
                w_recv.at[c, my_slot], partner,
            ).wait_send()

    @pl.when(is_inner)
    def _():
        @pl.loop(0, chunks)
        def _(c):
            for i in range(h):
                back_copy(i, c).wait_send()

        for j, (dist, _) in enumerate(inner_peers):
            for c in range(split):
                f_copy(c, j, dist).wait_send()
            for c in range(early):
                e_copy(c, j, dist).wait_send()

    @pl.when(jnp.logical_not(is_inner))
    def _():
        for j, (dist, inner) in enumerate(outer_peers):
            for c in range(early, chunks):
                f_copy(c, j, dist).wait_send()
            for c in range(split, chunks) if inner else range(early):
                e_copy(c, j, dist).wait_send()

    store(0, momentum_new, momentum_out).wait()
    store(1, outer_new, outer_out).wait()
    store(2, local_new, local_out).wait()

    @pl.loop(0, per_weight)
    def _(c):
        result_copy(keys, keys_out, c, 3 + c).wait()
        result_copy(values, values_out, c, 3 + per_weight + c).wait()


def per_device(
    groups, replicas,
    hidden_states, norm_gain, key_weight, value_weight, deltas, outer_params, momentum, local_params,
):
    hs, kw, vw = hidden_states[0], key_weight[0], value_weight[0]
    tokens, features = hs.shape
    depth, kv = kw.shape
    width = 2 * HEAD
    chunks = 2 * kv // width
    h = groups // 2
    half_depth = groups * depth
    cosine, sine = rotation_tables(tokens, HEAD)
    own = outer_params.shape
    vmem = pl.BlockSpec(memory_space=pltpu.VMEM)
    hbm = pl.BlockSpec(memory_space=pl.ANY)
    dma = pltpu.SemaphoreType.DMA
    bf16, f32 = jnp.bfloat16, jnp.float32
    results = pl.pallas_call(
        functools.partial(kernel, groups, replicas, width),
        out_shape=(
            jax.ShapeDtypeStruct((tokens, kv), bf16),
            jax.ShapeDtypeStruct((tokens, kv), bf16),
            jax.ShapeDtypeStruct(own, f32),
            jax.ShapeDtypeStruct(own, f32),
            jax.ShapeDtypeStruct(local_params.shape[1:], bf16),
        ),
        in_specs=[hbm, vmem] + [hbm] * 8,
        out_specs=[hbm] * 5,
        scratch_shapes=[
            pltpu.VMEM(cosine.shape, f32),
            pltpu.VMEM(sine.shape, f32),
            pltpu.VMEM(own, f32),
            pltpu.VMEM(own, f32),
            pltpu.VMEM(own, f32),
            pltpu.VMEM(local_params.shape[1:], bf16),
            pltpu.VMEM((tokens, kv), bf16),
            pltpu.VMEM((tokens, kv), bf16),
            pltpu.VMEM(own, f32),
            pltpu.VMEM(own, f32),
            pltpu.VMEM(local_params.shape[1:], bf16),
            pltpu.VMEM((tokens, features), bf16),
            pltpu.VMEM((2 * h, 1, depth), bf16),
            pltpu.VMEM((h, tokens, half_depth), bf16),
            pltpu.VMEM((h, tokens, half_depth), bf16),
            pltpu.VMEM((tokens, half_depth), bf16),
            pltpu.VMEM((chunks, half_depth, width), bf16),
            pltpu.VMEM((tokens, HEAD), f32),
            pltpu.VMEM((chunks, tokens, width), f32),
            pltpu.VMEM((h, chunks, tokens, width), bf16),
            pltpu.VMEM((chunks, tokens, width), bf16),
            pltpu.VMEM((replicas - 1,) + own, f32),
            pltpu.VMEM((replicas - 1,) + own, f32),
            dma,
            dma((4 * h - 1,)),
            dma((1 + h,)),
            dma((chunks,)),
            dma((chunks, 2 * h)),
            dma((chunks,)),
            dma((h - 1, chunks)),
            dma((h - 1, chunks)),
            dma((h - 1, chunks)),
            dma((h, chunks)),
            dma((chunks,)),
            dma((2, replicas - 1)),
            dma((2, replicas - 1)),
            dma((6,)),
            dma((3 + chunks,)),
        ],
        compiler_params=pltpu.CompilerParams(
            collective_id=0, has_side_effects=True, vmem_limit_bytes=60 * 1024 * 1024
        ),
    )(
        hs, norm_gain, kw, vw, cosine, sine,
        deltas[0], outer_params, momentum, local_params[0],
    )
    keys, values, momentum_new, outer_new, local_new = pl.pallas_call(
        write_out,
        out_shape=tuple(jax.ShapeDtypeStruct(a.shape, a.dtype) for a in results),
        in_specs=[vmem] * 5,
        out_specs=[hbm] * 5,
        scratch_shapes=[dma((5,))],
        compiler_params=pltpu.CompilerParams(vmem_limit_bytes=60 * 1024 * 1024),
    )(*results)
    return keys[None], values[None], momentum_new, outer_new, local_new[None]


def solution(mesh):
    in_specs = (
        P("replica", "fsdp", None),
        P("replica", "fsdp"),
        P("replica", "fsdp", None),
        P("replica", "fsdp", None),
        P("replica", "fsdp", None),
        P("fsdp", "replica"),
        P("fsdp", "replica"),
        P("replica", "fsdp", None),
    )
    out_specs = (
        P("replica", "fsdp", None),
        P("replica", "fsdp", None),
        P("fsdp", "replica"),
        P("fsdp", "replica"),
        P("replica", "fsdp", None),
    )
    groups, replicas = mesh.shape["fsdp"] // 2, mesh.shape["replica"]
    return jax.shard_map(
        functools.partial(per_device, groups, replicas),
        mesh=mesh, in_specs=in_specs, out_specs=out_specs, check_vma=False,
    )
```

```python
import functools

import jax
import jax.numpy as jnp
import numpy as np
from jax import lax
from jax.experimental import pallas as pl
from jax.experimental.pallas import tpu as pltpu
from jax.sharding import PartitionSpec as P

HEAD = 128
MESH = pl.DeviceIdType.MESH


def rotation_tables(tokens, head_size):
    half_width = head_size // 2
    exponent = np.arange(half_width, dtype=np.float32) * np.float32(2.0 / head_size)
    frequency = np.power(np.float32(500000.0), -exponent)
    angles = np.arange(tokens, dtype=np.float32)[:, None] * frequency[None, :]
    cosine, sine = np.cos(angles), np.sin(angles)
    return (
        jnp.asarray(np.concatenate([cosine, cosine], axis=1)),
        jnp.asarray(np.concatenate([-sine, sine], axis=1)),
    )


def write_out(*refs):
    count = len(refs) // 2
    sems = refs[-1]
    copies = [
        pltpu.make_async_copy(refs[i], refs[count + i], sems.at[i]) for i in range(count)
    ]
    for copy in copies:
        copy.start()
    for copy in copies:
        copy.wait()


def kernel(
    groups, replicas, width,
    hs, gain, kw, vw, cosine_in, sine_in, deltas, outer_in, momentum_in, local_in,
    keys, values, momentum_new, outer_new, local_new,
    cosine, sine, deltas_own, outer, momentum, local,
    hs_v, gains, a_in, a_scaled, a_own, weights, inv, acc, c_out, c_in, d_in, o_in,
    hs_sem, g_sem, a_sem, own_sem, w_recv, x_send, z_send, f_send, e_send,
    c_send, c_recv, d_sem, o_sem, load_sem,
):
    h = groups // 2
    r, f = lax.axis_index("replica"), lax.axis_index("fsdp")
    x, g = lax.rem(f, 2), lax.div(f, 2)
    half = lax.div(g, h)
    local_g = lax.rem(g, h)
    d = (h - 1 - local_g) * (1 - half) + local_g * half
    tokens, depth = hs.shape[0], kw.shape[0]
    half_depth = 2 * h * depth
    per_weight = kw.shape[1] // width
    chunks = 2 * per_weight
    first = chunks // 2
    split = chunks - chunks // 4
    early = chunks // 4
    own_w = outer.shape[1]
    features = hs.shape[1]

    def place(dist):
        return (h - 1 - dist) * (1 - half) + dist * half

    def slot(dist, side):
        return 2 * place(dist) + side

    def device(dist, side):
        return {"fsdp": 2 * (half * h + place(dist)) + side}

    def other_half(dist):
        return {"fsdp": 2 * ((1 - half) * (h + dist) + half * (h - 1 - dist)) + x}

    partner = device(d, 1 - x)
    outer_peers = [(0, True)] + [(1 + lax.rem(d - 1 + j, h - 1), False) for j in range(1, h - 1)]
    inner_peers = [(j, False) for j in range(1, h)]
    is_inner = d == 0

    def replica_at(j):
        return lax.rem(r + j, replicas)

    def mates():
        me = 2 * local_g + x
        return [
            {"fsdp": half * 2 * h + lax.rem(me + j, 2 * h)} for j in range(1, 2 * h)
        ]

    barrier = pltpu.get_barrier_semaphore()

    def greet(target):
        pl.semaphore_signal(barrier, inc=1, device_id=target, device_id_type=MESH)

    for target in mates():
        greet(target)
    greet(other_half(0))
    for j in range(1, replicas):
        greet({"replica": replica_at(j)})

    @pl.when(is_inner)
    def _():
        for i in range(h):
            greet(other_half(i))

    def remote(src, dst, send, recv, target):
        return pltpu.make_async_remote_copy(
            src_ref=src, dst_ref=dst, send_sem=send, recv_sem=recv,
            device_id=target, device_id_type=MESH,
        )

    mine = pl.ds(pl.multiple_of(r * own_w, own_w), own_w)
    hs_copy = pltpu.make_async_copy(hs, hs_v, hs_sem.at[0])
    hs_copy.start()
    my_slot = slot(d, x)
    partner_slot = slot(d, 1 - x)

    gain_copy = pltpu.make_async_copy(gain, gains.at[my_slot], hs_sem.at[1])
    gain_copy.start()

    def rows(q):
        return pl.ds(pl.multiple_of(q * depth, depth), depth)

    def source(c):
        return (kw if c < per_weight else vw).at[:, pl.ds((c % per_weight) * width, width)]

    own_copies = []
    for c in range(chunks):
        own_copies.append(
            pltpu.make_async_copy(source(c), weights.at[c, rows(my_slot)], own_sem.at[c])
        )
        own_copies[-1].start()
    loads = [
        pltpu.make_async_copy(src, dst, load_sem.at[i])
        for i, (src, dst) in enumerate(
            (
                (deltas.at[:, mine], deltas_own),
                (outer_in, outer),
                (momentum_in, momentum),
                (local_in, local),
                (cosine_in, cosine),
                (sine_in, sine),
            )
        )
    ]

    hs_copy.wait()
    pl.semaphore_wait(
        barrier, (2 * h - 1) + 1 + (replicas - 1) + jnp.where(is_inner, h, 0)
    )

    def x_copy(c):
        return remote(
            source(c), weights.at[c, rows(my_slot)], x_send.at[c], w_recv.at[c, my_slot], partner
        )

    def z_copy(c, j, dist):
        return remote(
            source(c), weights.at[c, rows(my_slot)], z_send.at[j, c], w_recv.at[c, my_slot],
            device(dist, x),
        )

    def f_copy(c, j, dist):
        q = slot(dist, x)
        return remote(
            weights.at[c, rows(q)], weights.at[c, rows(q)], f_send.at[j, c], w_recv.at[c, q],
            partner,
        )

    def e_copy(c, j, dist):
        return remote(
            weights.at[c, rows(partner_slot)], weights.at[c, rows(partner_slot)],
            e_send.at[j, c], w_recv.at[c, partner_slot], device(dist, x),
        )

    def arrived(c, q):
        remote(
            kw.at[:, pl.ds(0, width)], weights.at[c, rows(q)], x_send.at[0], w_recv.at[c, q],
            partner,
        ).wait_recv()

    g_copies = []
    for j, target in enumerate(mates()):
        g_copies.append(
            remote(gain, gains.at[my_slot], g_sem.at[j], g_sem.at[2 * h - 1 + my_slot], target)
        )
        g_copies[-1].start()

    away = pl.ds(pl.multiple_of((1 - half) * half_depth, half_depth), half_depth)
    a_copy = remote(hs_v.at[:, away], a_in.at[d], a_sem.at[0], a_sem.at[1 + d], other_half(0))

    @pl.when(is_inner)
    def _():
        for c in range(2):
            x_copy(c).start()
        a_copy.start()
        for c in range(chunks):
            for j, (dist, _) in enumerate(inner_peers):
                z_copy(c, j, dist).start()

    @pl.when(jnp.logical_not(is_inner))
    def _():
        for c in range(chunks):
            if c == first:
                a_copy.start()
            for j, (dist, _) in enumerate(outer_peers):
                z_copy(c, j, dist).start()
        for c in list(range(split, chunks)) + list(range(early)):
            x_copy(c).start()

    d_copies = []
    for j in range(1, replicas):
        columns = pl.ds(pl.multiple_of(replica_at(j) * own_w, own_w), own_w)
        d_copies.append(
            remote(
                deltas.at[:, columns], d_in.at[j - 1], d_sem.at[0, j - 1], d_sem.at[1, j - 1],
                {"replica": replica_at(j)},
            )
        )
        d_copies[-1].start()
    for copy in loads:
        copy.start()

    total = jnp.zeros((tokens, 1), jnp.float32)
    part_w = 2 * depth
    for k in range(features // part_w):
        part = hs_v[:, k * part_w : (k + 1) * part_w].astype(jnp.float32)
        total += jnp.sum(part * part, axis=1, keepdims=True)
    inv[...] = jnp.broadcast_to(lax.rsqrt(total / features + 1e-05), inv.shape)

    gain_copy.wait()
    for j in range(1, 2 * h):
        q = lax.rem(my_slot + j, 2 * h)
        remote(gain, gains.at[q], g_sem.at[0], g_sem.at[2 * h - 1 + q], partner).wait_recv()

    def scale(target, origin, base):
        for q in range(2 * h):
            at = pl.ds(base + q * depth, depth)
            target[:, q * depth : (q + 1) * depth] = (
                origin[:, at].astype(jnp.float32) * gains[q].astype(jnp.float32)
            ).astype(jnp.bfloat16)

    @pl.when(half == 0)
    def _():
        scale(a_own, hs_v, 0)

    @pl.when(half == 1)
    def _():
        scale(a_own, hs_v, half_depth)

    def own_product(c):
        acc[c] = jnp.dot(a_own[...], weights[c], preferred_element_type=jnp.float32)

    def back_copy(i, c):
        return remote(c_out.at[i, c], c_in.at[c], c_send.at[i, c], c_recv.at[c], other_half(i))

    def away_product(i, c):
        c_out[i, c] = jnp.dot(
            a_scaled[i], weights[c], preferred_element_type=jnp.float32
        ).astype(jnp.bfloat16)
        back_copy(i, c).start()

    def own_wait(c):
        pltpu.make_async_copy(
            kw.at[:, pl.ds(0, width)], weights.at[c, rows(my_slot)], own_sem.at[c]
        ).wait()

    def outer_step():
        for copy in loads:
            copy.wait()
        avg = deltas_own[...]
        for j in range(1, replicas):
            d_copies[j - 1].wait_recv()
            avg += d_in[j - 1]
        avg = avg / replicas
        moved = 0.9 * momentum[...] + avg
        momentum_new[...] = moved
        outer_new[...] = outer[...] - 0.7 * (avg + 0.9 * moved)
        for j in range(1, replicas):
            o_copy(j).start()

    def merge_step():
        part = jnp.float32(0.5)
        local_new[:, mine] = (
            part * local[:, mine].astype(jnp.float32) + part * outer_new[...]
        ).astype(jnp.bfloat16)
        for j in range(1, replicas):
            o_copy(j).wait_recv()
            theirs = pl.ds(
                pl.multiple_of(lax.rem(r + replicas - j, replicas) * own_w, own_w), own_w
            )
            local_new[:, theirs] = (
                part * local[:, theirs].astype(jnp.float32) + part * o_in[j - 1]
            ).astype(jnp.bfloat16)

    def o_copy(j):
        return remote(
            outer_new, o_in.at[j - 1], o_sem.at[0, j - 1], o_sem.at[1, j - 1],
            {"replica": replica_at(j)},
        )

    @pl.when(is_inner)
    def _():
        def pass_on(c):
            for j, (dist, _) in enumerate(inner_peers):
                arrived(c, slot(dist, x))
                if c < split:
                    f_copy(c, j, dist).start()

        for c in range(first):
            pass_on(c)
            if c + 2 < first:
                x_copy(c + 2).start()
            if c < early:
                arrived(c, partner_slot)
                for j, (dist, _) in enumerate(inner_peers):
                    e_copy(c, j, dist).start()
            if c == 0:
                outer_step()
            if c == 1:
                merge_step()
        for c in range(first, split):
            x_copy(c).start()

        def rest(c, known):
            own_wait(c)
            if not known:
                arrived(c, partner_slot)
            for dist, _ in inner_peers:
                arrived(c, slot(dist, 1 - x))

        remote(hs.at[:, away], a_in.at[0], a_sem.at[0], a_sem.at[1], partner).wait_recv()
        for q in range(2 * h):
            at = slice(q * depth, (q + 1) * depth)
            a_scaled[0, :, at] = (
                a_in[0, :, at].astype(jnp.float32) * gains[q].astype(jnp.float32)
            ).astype(jnp.bfloat16)

        @pl.loop(0, early)
        def _(c):
            rest(c, True)
            away_product(0, c)
            own_product(c)

        @pl.loop(early, first)
        def _(c):
            rest(c, False)
            away_product(0, c)
            own_product(c)

        for i in range(1, h):
            remote(
                hs.at[:, away], a_in.at[i], a_sem.at[0], a_sem.at[1 + i], partner
            ).wait_recv()
            for q in range(2 * h):
                at = slice(q * depth, (q + 1) * depth)
                a_scaled[i, :, at] = (
                    a_in[i, :, at].astype(jnp.float32) * gains[q].astype(jnp.float32)
                ).astype(jnp.bfloat16)

            @pl.loop(0, first)
            def _(c):
                away_product(i, c)

        pass_on(first)
        for c in range(first, chunks):
            if c + 1 < chunks:
                pass_on(c + 1)
            if c + 1 == split - 1:
                for k in range(split, chunks):
                    x_copy(k).start()
            rest(c, False)
            for i in reversed(range(h)):
                away_product(i, c)
            own_product(c)

    @pl.when(jnp.logical_not(is_inner))
    def _():
        for c in range(chunks):
            for j, (dist, _) in enumerate(outer_peers):
                arrived(c, slot(dist, x))
                if c >= early:
                    f_copy(c, j, dist).start()
            if early <= c < split:
                x_copy(c).start()
            if c == 1:
                for k in range(split, chunks):
                    arrived(k, partner_slot)
                    for j, (dist, inner) in enumerate(outer_peers):
                        if inner:
                            e_copy(k, j, dist).start()
                outer_step()
            if c == 2:
                for k in range(early):
                    arrived(k, partner_slot)
                    for j, (dist, inner) in enumerate(outer_peers):
                        if not inner:
                            e_copy(k, j, dist).start()
                merge_step()

        def finish(c, known):
            own_wait(c)
            if not known:
                arrived(c, partner_slot)
            for dist, _ in outer_peers:
                arrived(c, slot(dist, 1 - x))
            own_product(c)

        @pl.loop(early, split)
        def _(c):
            finish(c, False)

        @pl.loop(0, early)
        def _(c):
            finish(c, True)

        @pl.loop(split, chunks)
        def _(c):
            finish(c, True)

    def summed(c):
        back_copy(0, c).wait_recv()
        return (acc[c] + c_in[c].astype(jnp.float32)) * inv[:, 0:1]

    @pl.loop(0, per_weight)
    def _(c):
        value = summed(c)
        for k in range(width // HEAD):
            head = value[:, k * HEAD : (k + 1) * HEAD]
            turned = head * cosine[...] + pltpu.roll(head, HEAD // 2, 1) * sine[...]
            at = pl.ds(pl.multiple_of(c * width + k * HEAD, HEAD), HEAD)
            keys[:, at] = turned.astype(jnp.bfloat16)

    @pl.loop(0, per_weight)
    def _(c):
        at = pl.ds(pl.multiple_of(c * width, width), width)
        values[:, at] = summed(c + per_weight).astype(jnp.bfloat16)

    a_copy.wait_send()
    for copy in g_copies + d_copies:
        copy.wait_send()
    for j in range(1, replicas):
        o_copy(j).wait_send()

    @pl.loop(0, chunks)
    def _(c):
        remote(
            kw.at[:, pl.ds(0, width)], weights.at[c, rows(my_slot)], x_send.at[c],
            w_recv.at[c, my_slot], partner,
        ).wait_send()
        for j in range(h - 1):
            remote(
                kw.at[:, pl.ds(0, width)], weights.at[c, rows(my_slot)], z_send.at[j, c],
                w_recv.at[c, my_slot], partner,
            ).wait_send()

    @pl.when(is_inner)
    def _():
        @pl.loop(0, chunks)
        def _(c):
            for i in range(h):
                back_copy(i, c).wait_send()

        for j, (dist, _) in enumerate(inner_peers):
            for c in range(split):
                f_copy(c, j, dist).wait_send()
            for c in range(early):
                e_copy(c, j, dist).wait_send()

    @pl.when(jnp.logical_not(is_inner))
    def _():
        for j, (dist, inner) in enumerate(outer_peers):
            for c in range(early, chunks):
                f_copy(c, j, dist).wait_send()
            for c in range(split, chunks) if inner else range(early):
                e_copy(c, j, dist).wait_send()


def per_device(
    groups, replicas,
    hidden_states, norm_gain, key_weight, value_weight, deltas, outer_params, momentum, local_params,
):
    hs, kw, vw = hidden_states[0], key_weight[0], value_weight[0]
    tokens, features = hs.shape
    depth, kv = kw.shape
    width = 2 * HEAD
    chunks = 2 * kv // width
    h = groups // 2
    half_depth = groups * depth
    cosine, sine = rotation_tables(tokens, HEAD)
    own = outer_params.shape
    vmem = pl.BlockSpec(memory_space=pltpu.VMEM)
    hbm = pl.BlockSpec(memory_space=pl.ANY)
    dma = pltpu.SemaphoreType.DMA
    bf16, f32 = jnp.bfloat16, jnp.float32
    results = pl.pallas_call(
        functools.partial(kernel, groups, replicas, width),
        out_shape=(
            pltpu.VMEM((tokens, kv), bf16),
            pltpu.VMEM((tokens, kv), bf16),
            pltpu.VMEM(own, f32),
            pltpu.VMEM(own, f32),
            pltpu.VMEM(local_params.shape[1:], bf16),
        ),
        in_specs=[hbm] * 10,
        out_specs=[vmem] * 5,
        scratch_shapes=[
            pltpu.VMEM(cosine.shape, f32),
            pltpu.VMEM(sine.shape, f32),
            pltpu.VMEM(own, f32),
            pltpu.VMEM(own, f32),
            pltpu.VMEM(own, f32),
            pltpu.VMEM(local_params.shape[1:], bf16),
            pltpu.VMEM((tokens, features), bf16),
            pltpu.VMEM((2 * h, 1, depth), bf16),
            pltpu.VMEM((h, tokens, half_depth), bf16),
            pltpu.VMEM((h, tokens, half_depth), bf16),
            pltpu.VMEM((tokens, half_depth), bf16),
            pltpu.VMEM((chunks, half_depth, width), bf16),
            pltpu.VMEM((tokens, HEAD), f32),
            pltpu.VMEM((chunks, tokens, width), f32),
            pltpu.VMEM((h, chunks, tokens, width), bf16),
            pltpu.VMEM((chunks, tokens, width), bf16),
            pltpu.VMEM((replicas - 1,) + own, f32),
            pltpu.VMEM((replicas - 1,) + own, f32),
            dma((2,)),
            dma((4 * h - 1,)),
            dma((1 + h,)),
            dma((chunks,)),
            dma((chunks, 2 * h)),
            dma((chunks,)),
            dma((h - 1, chunks)),
            dma((h - 1, chunks)),
            dma((h - 1, chunks)),
            dma((h, chunks)),
            dma((chunks,)),
            dma((2, replicas - 1)),
            dma((2, replicas - 1)),
            dma((6,)),
        ],
        compiler_params=pltpu.CompilerParams(
            collective_id=0, has_side_effects=True, vmem_limit_bytes=60 * 1024 * 1024
        ),
    )(
        hs, norm_gain, kw, vw, cosine, sine,
        deltas[0], outer_params, momentum, local_params[0],
    )
    keys, values, momentum_new, outer_new, local_new = pl.pallas_call(
        write_out,
        out_shape=tuple(jax.ShapeDtypeStruct(a.shape, a.dtype) for a in results),
        in_specs=[vmem] * 5,
        out_specs=[hbm] * 5,
        scratch_shapes=[dma((5,))],
        compiler_params=pltpu.CompilerParams(vmem_limit_bytes=1024 * 1024),
    )(*results)
    return keys[None], values[None], momentum_new, outer_new, local_new[None]


def solution(mesh):
    in_specs = (
        P("replica", "fsdp", None),
        P("replica", "fsdp"),
        P("replica", "fsdp", None),
        P("replica", "fsdp", None),
        P("replica", "fsdp", None),
        P("fsdp", "replica"),
        P("fsdp", "replica"),
        P("replica", "fsdp", None),
    )
    out_specs = (
        P("replica", "fsdp", None),
        P("replica", "fsdp", None),
        P("fsdp", "replica"),
        P("fsdp", "replica"),
        P("replica", "fsdp", None),
    )
    groups, replicas = mesh.shape["fsdp"] // 2, mesh.shape["replica"]
    return jax.shard_map(
        functools.partial(per_device, groups, replicas),
        mesh=mesh, in_specs=in_specs, out_specs=out_specs, check_vma=False,
    )
```

```python
import functools

import jax
import jax.numpy as jnp
import numpy as np
from jax import lax
from jax.experimental import pallas as pl
from jax.experimental.pallas import tpu as pltpu
from jax.sharding import PartitionSpec as P

HEAD = 128
MESH = pl.DeviceIdType.MESH


def rotation_tables(tokens, head_size):
    half_width = head_size // 2
    exponent = np.arange(half_width, dtype=np.float32) * np.float32(2.0 / head_size)
    frequency = np.power(np.float32(500000.0), -exponent)
    angles = np.arange(tokens, dtype=np.float32)[:, None] * frequency[None, :]
    cosine, sine = np.cos(angles), np.sin(angles)
    return (
        jnp.asarray(np.concatenate([cosine, cosine], axis=1)),
        jnp.asarray(np.concatenate([-sine, sine], axis=1)),
    )


def write_out(*refs):
    count = len(refs) // 2
    sems = refs[-1]
    copies = [
        pltpu.make_async_copy(refs[i], refs[count + i], sems.at[i]) for i in range(count)
    ]
    for copy in copies:
        copy.start()
    for copy in copies:
        copy.wait()


def kernel(
    groups, replicas, width,
    hs, gain, kw, vw, cosine_in, sine_in, deltas, outer_in, momentum_in, local_in,
    keys, values, momentum_new, outer_new, local_new,
    rotation, state, local,
    hs_v, gains, a_in, a_scaled, a_own, weights, inv, acc, c_out, c_in, d_in, o_in,
    hs_sem, g_sem, g_recv, a_sem, z_recv, p_recv, w_recv, x_send, z_send, f_send, e_send,
    c_send, c_recv, d_sem, o_sem, load_sem,
):
    h = groups // 2
    r, f = lax.axis_index("replica"), lax.axis_index("fsdp")
    x, g = lax.rem(f, 2), lax.div(f, 2)
    half = lax.div(g, h)
    local_g = lax.rem(g, h)
    d = (h - 1 - local_g) * (1 - half) + local_g * half
    tokens, depth = hs.shape[0], kw.shape[0]
    half_depth = 2 * h * depth
    per_weight = kw.shape[1] // width
    chunks = 2 * per_weight
    first = chunks // 2
    split = chunks - chunks // 4
    early = chunks // 4
    own_w = outer_in.shape[1]
    cosine, sine = rotation.at[0], rotation.at[1]
    deltas_own, outer, momentum = state.at[0], state.at[1], state.at[2]
    features = hs.shape[1]

    def place(dist):
        return (h - 1 - dist) * (1 - half) + dist * half

    def slot(dist, side):
        return 2 * place(dist) + side

    def device(dist, side):
        return {"fsdp": 2 * (half * h + place(dist)) + side}

    def other_half(dist):
        return {"fsdp": 2 * ((1 - half) * (h + dist) + half * (h - 1 - dist)) + x}

    partner = device(d, 1 - x)
    outer_peers = [(0, True)] + [(1 + lax.rem(d - 1 + j, h - 1), False) for j in range(1, h - 1)]
    inner_peers = [(j, False) for j in range(1, h)]
    is_inner = d == 0

    def replica_at(j):
        return lax.rem(r + j, replicas)

    barrier = pltpu.get_barrier_semaphore()

    def greet(target):
        pl.semaphore_signal(barrier, inc=1, device_id=target, device_id_type=MESH)

    greet(partner)
    for j in range(1, replicas):
        greet({"replica": replica_at(j)})

    @pl.when(is_inner)
    def _():
        for i in range(h):
            greet(other_half(i))
        for dist, _ in inner_peers:
            greet(device(dist, x))

    @pl.when(jnp.logical_not(is_inner))
    def _():
        for dist, _ in outer_peers:
            greet(device(dist, x))

    def remote(src, dst, send, recv, target):
        return pltpu.make_async_remote_copy(
            src_ref=src, dst_ref=dst, send_sem=send, recv_sem=recv,
            device_id=target, device_id_type=MESH,
        )

    mine = pl.ds(pl.multiple_of(r * own_w, own_w), own_w)
    away = pl.ds(pl.multiple_of((1 - half) * half_depth, half_depth), half_depth)
    home = pl.ds(pl.multiple_of(half * half_depth, half_depth), half_depth)
    hs_copy = pltpu.make_async_copy(hs.at[:, away], hs_v.at[:, away], hs_sem.at[0])
    hs_copy.start()
    home_copy = pltpu.make_async_copy(hs.at[:, home], hs_v.at[:, home], hs_sem.at[1])
    my_slot = slot(d, x)
    partner_slot = slot(d, 1 - x)

    def rows(q):
        return pl.ds(pl.multiple_of(q * depth, depth), depth)

    def source(c):
        return (kw if c < per_weight else vw).at[:, pl.ds((c % per_weight) * width, width)]

    own_copies = [
        pltpu.make_async_copy(source(c), weights.at[c, rows(my_slot)], w_recv.at[c])
        for c in range(chunks)
    ]
    loads = [
        pltpu.make_async_copy(src, dst, load_sem.at[i])
        for i, src, dst in (
            (0, deltas.at[:, mine], deltas_own),
            (0, outer_in, outer),
            (0, momentum_in, momentum),
            (1, cosine_in, cosine),
            (1, sine_in, sine),
            (2, local_in, local),
        )
    ]

    hs_copy.wait()
    pl.semaphore_wait(barrier, 1 + (h - 1) + 1 + (replicas - 1))

    def heard(sender, receiver):
        return lax.rem(sender - receiver - 1 + h, h)

    def x_copy(c, known):
        arrival = w_recv.at[c] if known is None else p_recv.at[known]
        return remote(source(c), weights.at[c, rows(my_slot)], x_send, arrival, partner)

    def z_copy(c, j, dist):
        return remote(
            source(c), weights.at[c, rows(my_slot)], z_send.at[j], z_recv.at[heard(d, dist), c],
            device(dist, x),
        )

    def f_copy(c, j, dist):
        at = weights.at[c, rows(slot(dist, x))]
        return remote(at, at, f_send.at[j], w_recv.at[c], partner)

    def e_copy(c, j, dist):
        at = weights.at[c, rows(partner_slot)]
        return remote(at, at, e_send.at[j], w_recv.at[c], device(dist, x))

    def landed(ref, sem):
        remote(ref, ref, x_send, sem, partner).wait_recv()

    def left(ref, sem):
        remote(ref, ref, sem, w_recv.at[0], partner).wait_send()

    def from_peer(c, dist):
        landed(weights.at[c, rows(slot(dist, x))], z_recv.at[heard(dist, d), c])

    def from_partner(c, known):
        landed(weights.at[c, rows(partner_slot)], p_recv.at[known])

    def rest(c, known):
        count = h if known else h + 1
        landed(weights.at[c, pl.ds(0, count * depth)], w_recv.at[c])

    def send_gain(peers):
        remote(gain, gains.at[my_slot], g_sem, g_recv.at[h - 1], partner).start()
        for dist, _ in peers:
            remote(
                gain, gains.at[my_slot], g_sem, g_recv.at[heard(d, dist)], device(dist, x)
            ).start()

    def pass_gain(peers):
        for dist, _ in peers:
            at = gains.at[slot(dist, x)]
            landed(at, g_recv.at[heard(dist, d)])
            remote(at, at, g_sem, g_recv.at[h - 1], partner).start()

    a_copy = remote(hs_v.at[:, away], a_in.at[d], a_sem.at[0], a_sem.at[1 + d], other_half(0))

    @pl.when(is_inner)
    def _():
        a_copy.start()
        send_gain(inner_peers)
        for c in range(2):
            x_copy(c, c if c < early else None).start()
        for c in range(chunks):
            for j, (dist, _) in enumerate(inner_peers):
                z_copy(c, j, dist).start()

    @pl.when(jnp.logical_not(is_inner))
    def _():
        send_gain(outer_peers)
        for c in range(chunks):
            if c == first:
                a_copy.start()
            for j, (dist, _) in enumerate(outer_peers):
                z_copy(c, j, dist).start()
        for c in list(range(split, chunks)) + list(range(early)):
            x_copy(c, c - split if c >= split else None).start()

    gain_copy = pltpu.make_async_copy(gain, gains.at[my_slot], g_recv.at[h - 1])
    gain_copy.start()
    home_copy.start()
    for j in range(1, replicas):
        columns = pl.ds(pl.multiple_of(replica_at(j) * own_w, own_w), own_w)
        remote(
            deltas.at[:, columns], d_in.at[j - 1], d_sem.at[0], d_sem.at[1],
            {"replica": replica_at(j)},
        ).start()
    for copy in loads + own_copies:
        copy.start()

    home_copy.wait()
    total = jnp.zeros((tokens, 1), jnp.float32)
    part_w = 2 * depth
    for k in range(features // part_w):
        part = hs_v[:, k * part_w : (k + 1) * part_w].astype(jnp.float32)
        total += jnp.sum(part * part, axis=1, keepdims=True)
    inv[...] = jnp.broadcast_to(lax.rsqrt(total / features + 1e-05), inv.shape)

    @pl.when(is_inner)
    def _():
        pass_gain(inner_peers)

    @pl.when(jnp.logical_not(is_inner))
    def _():
        pass_gain(outer_peers)

    landed(gains.at[pl.ds(0, h + 1)], g_recv.at[h - 1])

    def scale(target, origin, base):
        for q in range(2 * h):
            at = pl.ds(base + q * depth, depth)
            target[:, q * depth : (q + 1) * depth] = (
                origin[:, at].astype(jnp.float32) * gains[q].astype(jnp.float32)
            ).astype(jnp.bfloat16)

    @pl.when(half == 0)
    def _():
        scale(a_own, hs_v, 0)

    @pl.when(half == 1)
    def _():
        scale(a_own, hs_v, half_depth)

    def own_product(c):
        acc[c] = jnp.dot(a_own[...], weights[c], preferred_element_type=jnp.float32)

    def away_product(i, c, final=False):
        c_out[i, c] = jnp.dot(
            a_scaled[i], weights[c], preferred_element_type=jnp.float32
        ).astype(jnp.bfloat16)
        remote(
            c_out.at[i, c], c_in.at[c], c_send, c_recv.at[1 if final else 0], other_half(i)
        ).start()

    def outer_step():
        pltpu.make_async_copy(state, state, load_sem.at[0]).wait()
        landed(d_in, d_sem.at[1])
        avg = deltas_own[...]
        for j in range(1, replicas):
            avg += d_in[j - 1]
        avg = avg / replicas
        moved = 0.9 * momentum[...] + avg
        momentum_new[...] = moved
        outer_new[...] = outer[...] - 0.7 * (avg + 0.9 * moved)
        for j in range(1, replicas):
            remote(
                outer_new, o_in.at[j - 1], o_sem.at[0], o_sem.at[1], {"replica": replica_at(j)}
            ).start()

    def merge_step():
        part = jnp.float32(0.5)
        loads[-1].wait()
        local_new[:, mine] = (
            part * local[:, mine].astype(jnp.float32) + part * outer_new[...]
        ).astype(jnp.bfloat16)
        landed(o_in, o_sem.at[1])
        for j in range(1, replicas):
            theirs = pl.ds(
                pl.multiple_of(lax.rem(r + replicas - j, replicas) * own_w, own_w), own_w
            )
            local_new[:, theirs] = (
                part * local[:, theirs].astype(jnp.float32) + part * o_in[j - 1]
            ).astype(jnp.bfloat16)

    @pl.when(is_inner)
    def _():
        def pass_on(c):
            for j, (dist, _) in enumerate(inner_peers):
                from_peer(c, dist)
                if c < split:
                    f_copy(c, j, dist).start()

        for c in range(first):
            pass_on(c)
            if c + 2 < first:
                x_copy(c + 2, None).start()
            if c < early:
                from_partner(c, c)
                for j, (dist, _) in enumerate(inner_peers):
                    e_copy(c, j, dist).start()
            if c == 0:
                outer_step()
            if c == 1:
                merge_step()
        for c in range(first, split):
            x_copy(c, None).start()

        remote(hs.at[:, away], a_in.at[0], a_sem.at[0], a_sem.at[1], partner).wait_recv()
        for q in range(2 * h):
            at = slice(q * depth, (q + 1) * depth)
            a_scaled[0, :, at] = (
                a_in[0, :, at].astype(jnp.float32) * gains[q].astype(jnp.float32)
            ).astype(jnp.bfloat16)

        @pl.loop(0, early)
        def _(c):
            rest(c, True)
            away_product(0, c)
            own_product(c)

        @pl.loop(early, first)
        def _(c):
            rest(c, False)
            away_product(0, c)
            own_product(c)

        for i in range(1, h):
            remote(
                hs.at[:, away], a_in.at[i], a_sem.at[0], a_sem.at[1 + i], partner
            ).wait_recv()
            for q in range(2 * h):
                at = slice(q * depth, (q + 1) * depth)
                a_scaled[i, :, at] = (
                    a_in[i, :, at].astype(jnp.float32) * gains[q].astype(jnp.float32)
                ).astype(jnp.bfloat16)

            @pl.loop(0, first)
            def _(c):
                away_product(i, c)

        pass_on(first)
        for c in range(first, chunks):
            if c + 1 < chunks:
                pass_on(c + 1)
            if c + 1 == split - 1:
                for k in range(split, chunks):
                    x_copy(k, None).start()
            rest(c, False)
            for i in reversed(range(h)):
                away_product(i, c, c == chunks - 1)
            own_product(c)

    @pl.when(jnp.logical_not(is_inner))
    def _():
        for c in range(chunks):
            for j, (dist, _) in enumerate(outer_peers):
                from_peer(c, dist)
                if c >= early:
                    f_copy(c, j, dist).start()
            if early <= c < split:
                x_copy(c, None).start()
            if c == 1:
                for k in range(split, chunks):
                    from_partner(k, k - split)
                    for j, (dist, inner) in enumerate(outer_peers):
                        if inner:
                            e_copy(k, j, dist).start()
                outer_step()
            if c == 2:
                merge_step()

        def finish(c, known):
            rest(c, known)
            own_product(c)

        @pl.loop(0, split)
        def _(c):
            finish(c, False)

        @pl.loop(split, chunks)
        def _(c):
            finish(c, True)

    landed(rotation, load_sem.at[1])

    def summed(c):
        return (acc[c] + c_in[c].astype(jnp.float32)) * inv[:, 0:1]

    landed(c_in.at[pl.ds(0, chunks - 1)], c_recv.at[0])

    @pl.loop(0, per_weight)
    def _(c):
        value = summed(c)
        for k in range(width // HEAD):
            head = value[:, k * HEAD : (k + 1) * HEAD]
            turned = head * cosine[...] + pltpu.roll(head, HEAD // 2, 1) * sine[...]
            at = pl.ds(pl.multiple_of(c * width + k * HEAD, HEAD), HEAD)
            keys[:, at] = turned.astype(jnp.bfloat16)

    @pl.loop(0, per_weight - 1)
    def _(c):
        at = pl.ds(pl.multiple_of(c * width, width), width)
        values[:, at] = summed(c + per_weight).astype(jnp.bfloat16)

    a_copy.wait_send()
    left(d_in, d_sem.at[0])
    left(o_in, o_sem.at[0])
    left(gains.at[pl.ds(0, 2 * h - 1)], g_sem)
    left(weights.at[:, rows(my_slot)], x_send)
    for j in range(h - 1):
        left(weights.at[:, rows(my_slot)], z_send.at[j])
        left(weights.at[pl.ds(0, split), rows(my_slot)], f_send.at[j])

    @pl.when(is_inner)
    def _():
        for j in range(h - 1):
            left(weights.at[pl.ds(0, early), rows(my_slot)], e_send.at[j])

    @pl.when(jnp.logical_not(is_inner))
    def _():
        left(weights.at[pl.ds(0, early), rows(my_slot)], e_send.at[0])

    landed(c_in.at[chunks - 1], c_recv.at[1])
    values[:, pl.ds((per_weight - 1) * width, width)] = summed(chunks - 1).astype(jnp.bfloat16)

    @pl.when(is_inner)
    def _():
        left(c_out, c_send)


def per_device(
    groups, replicas,
    hidden_states, norm_gain, key_weight, value_weight, deltas, outer_params, momentum, local_params,
):
    hs, kw, vw = hidden_states[0], key_weight[0], value_weight[0]
    tokens, features = hs.shape
    depth, kv = kw.shape
    width = 2 * HEAD
    chunks = 2 * kv // width
    h = groups // 2
    half_depth = groups * depth
    cosine, sine = rotation_tables(tokens, HEAD)
    own = outer_params.shape
    vmem = pl.BlockSpec(memory_space=pltpu.VMEM)
    hbm = pl.BlockSpec(memory_space=pl.ANY)
    dma = pltpu.SemaphoreType.DMA
    bf16, f32 = jnp.bfloat16, jnp.float32
    results = pl.pallas_call(
        functools.partial(kernel, groups, replicas, width),
        out_shape=(
            pltpu.VMEM((tokens, kv), bf16),
            pltpu.VMEM((tokens, kv), bf16),
            pltpu.VMEM(own, f32),
            pltpu.VMEM(own, f32),
            pltpu.VMEM(local_params.shape[1:], bf16),
        ),
        in_specs=[hbm] * 10,
        out_specs=[vmem] * 5,
        scratch_shapes=[
            pltpu.VMEM((2, tokens, HEAD), f32),
            pltpu.VMEM((3,) + own, f32),
            pltpu.VMEM(local_params.shape[1:], bf16),
            pltpu.VMEM((tokens, features), bf16),
            pltpu.VMEM((2 * h, 1, depth), bf16),
            pltpu.VMEM((h, tokens, half_depth), bf16),
            pltpu.VMEM((h, tokens, half_depth), bf16),
            pltpu.VMEM((tokens, half_depth), bf16),
            pltpu.VMEM((chunks, half_depth, width), bf16),
            pltpu.VMEM((tokens, HEAD), f32),
            pltpu.VMEM((chunks, tokens, width), f32),
            pltpu.VMEM((h, chunks, tokens, width), bf16),
            pltpu.VMEM((chunks, tokens, width), bf16),
            pltpu.VMEM((replicas - 1,) + own, f32),
            pltpu.VMEM((replicas - 1,) + own, f32),
            dma((2,)),
            dma,
            dma((h,)),
            dma((1 + h,)),
            dma((h - 1, chunks)),
            dma((chunks // 4,)),
            dma((chunks,)),
            dma,
            dma((h - 1,)),
            dma((h - 1,)),
            dma((h - 1,)),
            dma,
            dma((2,)),
            dma((2,)),
            dma((2,)),
            dma((3,)),
        ],
        compiler_params=pltpu.CompilerParams(
            collective_id=0, has_side_effects=True, vmem_limit_bytes=60 * 1024 * 1024
        ),
    )(
        hs, norm_gain, kw, vw, cosine, sine,
        deltas[0], outer_params, momentum, local_params[0],
    )
    keys, values, momentum_new, outer_new, local_new = pl.pallas_call(
        write_out,
        out_shape=tuple(jax.ShapeDtypeStruct(a.shape, a.dtype) for a in results),
        in_specs=[vmem] * 5,
        out_specs=[hbm] * 5,
        scratch_shapes=[dma((5,))],
        compiler_params=pltpu.CompilerParams(vmem_limit_bytes=1024 * 1024),
    )(*results)
    return keys[None], values[None], momentum_new, outer_new, local_new[None]


def solution(mesh):
    in_specs = (
        P("replica", "fsdp", None),
        P("replica", "fsdp"),
        P("replica", "fsdp", None),
        P("replica", "fsdp", None),
        P("replica", "fsdp", None),
        P("fsdp", "replica"),
        P("fsdp", "replica"),
        P("replica", "fsdp", None),
    )
    out_specs = (
        P("replica", "fsdp", None),
        P("replica", "fsdp", None),
        P("fsdp", "replica"),
        P("fsdp", "replica"),
        P("replica", "fsdp", None),
    )
    groups, replicas = mesh.shape["fsdp"] // 2, mesh.shape["replica"]
    return jax.shard_map(
        functools.partial(per_device, groups, replicas),
        mesh=mesh, in_specs=in_specs, out_specs=out_specs, check_vma=False,
    )
```

```python
import functools

import jax
import jax.numpy as jnp
import numpy as np
from jax import lax
from jax.experimental import pallas as pl
from jax.experimental.pallas import tpu as pltpu
from jax.sharding import PartitionSpec as P

HEAD = 128
MESH = pl.DeviceIdType.MESH


def rotation_tables(tokens, head_size):
    half_width = head_size // 2
    exponent = np.arange(half_width, dtype=np.float32) * np.float32(2.0 / head_size)
    frequency = np.power(np.float32(500000.0), -exponent)
    angles = np.arange(tokens, dtype=np.float32)[:, None] * frequency[None, :]
    cosine, sine = np.cos(angles), np.sin(angles)
    return (
        jnp.asarray(np.concatenate([cosine, cosine], axis=1)),
        jnp.asarray(np.concatenate([-sine, sine], axis=1)),
    )


def write_out(*refs):
    count = len(refs) // 2
    sems = refs[-1]
    copies = [
        pltpu.make_async_copy(refs[i], refs[count + i], sems.at[i]) for i in range(count)
    ]
    for copy in copies:
        copy.start()
    for copy in copies:
        copy.wait()


def kernel(
    groups, replicas, width,
    hs, gain, kw, vw, cosine_in, sine_in, deltas, outer_in, momentum_in, local_in,
    keys, values, momentum_new, outer_new, local_new,
    rotation, state, local, lead,
    hs_v, gains, a_in, a_scaled, a_own, weights, inv, acc, c_out, c_in, d_in, o_in,
    hs_sem, g_sem, g_recv, a_sem, z_recv, p_recv, w_recv, x_send, z_send, f_send, e_send,
    c_send, c_recv, d_sem, o_sem, load_sem,
):
    h = groups // 2
    r, f = lax.axis_index("replica"), lax.axis_index("fsdp")
    x, g = lax.rem(f, 2), lax.div(f, 2)
    half = lax.div(g, h)
    local_g = lax.rem(g, h)
    d = (h - 1 - local_g) * (1 - half) + local_g * half
    tokens, depth = hs.shape[0], kw.shape[0]
    half_depth = 2 * h * depth
    per_weight = kw.shape[1] // width
    chunks = 2 * per_weight
    first = chunks // 2 - 1
    split = chunks - chunks // 4
    early = chunks // 4
    own_w = outer_in.shape[1]
    cosine, sine = rotation.at[0], rotation.at[1]
    deltas_own, outer, momentum = state.at[0], state.at[1], state.at[2]
    features = hs.shape[1]

    def place(dist):
        return (h - 1 - dist) * (1 - half) + dist * half

    def slot(dist, side):
        return 2 * place(dist) + side

    def device(dist, side):
        return {"fsdp": 2 * (half * h + place(dist)) + side}

    def other_half(dist):
        return {"fsdp": 2 * ((1 - half) * (h + dist) + half * (h - 1 - dist)) + x}

    partner = device(d, 1 - x)
    outer_peers = [(0, True)] + [(1 + lax.rem(d - 1 + j, h - 1), False) for j in range(1, h - 1)]
    inner_peers = [(j, False) for j in range(1, h)]
    is_inner = d == 0

    def replica_at(j):
        return lax.rem(r + j, replicas)

    barrier = pltpu.get_barrier_semaphore()

    def greet(target):
        pl.semaphore_signal(barrier, inc=1, device_id=target, device_id_type=MESH)

    greet(partner)
    for j in range(1, replicas):
        greet({"replica": replica_at(j)})

    @pl.when(is_inner)
    def _():
        greet(other_half(0))
        for dist, _ in inner_peers:
            greet(device(dist, x))

    @pl.when(jnp.logical_not(is_inner))
    def _():
        for dist, _ in outer_peers:
            greet(device(dist, x))

    def remote(src, dst, send, recv, target):
        return pltpu.make_async_remote_copy(
            src_ref=src, dst_ref=dst, send_sem=send, recv_sem=recv,
            device_id=target, device_id_type=MESH,
        )

    mine = pl.ds(pl.multiple_of(r * own_w, own_w), own_w)
    away = pl.ds(pl.multiple_of((1 - half) * half_depth, half_depth), half_depth)
    home = pl.ds(pl.multiple_of(half * half_depth, half_depth), half_depth)
    hs_copy = pltpu.make_async_copy(hs.at[:, away], hs_v.at[:, away], hs_sem.at[0])
    hs_copy.start()
    lead_copy = pltpu.make_async_copy(kw.at[:, pl.ds(0, width)], lead, hs_sem.at[2])
    lead_copy.start()
    home_copy = pltpu.make_async_copy(hs.at[:, home], hs_v.at[:, home], hs_sem.at[1])
    my_slot = slot(d, x)
    partner_slot = slot(d, 1 - x)

    def rows(q):
        return pl.ds(pl.multiple_of(q * depth, depth), depth)

    def source(c):
        return (kw if c < per_weight else vw).at[:, pl.ds((c % per_weight) * width, width)]

    own_copies = [
        pltpu.make_async_copy(source(c), weights.at[c, rows(my_slot)], hs_sem.at[3])
        for c in range(chunks)
    ]
    loads = [
        pltpu.make_async_copy(src, dst, load_sem.at[i])
        for i, src, dst in (
            (0, deltas.at[:, mine], deltas_own),
            (0, outer_in, outer),
            (0, momentum_in, momentum),
            (1, cosine_in, cosine),
            (1, sine_in, sine),
            (2, local_in, local),
        )
    ]

    for copy in own_copies:
        copy.start()
    pl.semaphore_wait(barrier, 1 + (h - 1) + (replicas - 1) + jnp.where(is_inner, 1, 0))

    def heard(sender, receiver):
        return lax.rem(sender - receiver - 1 + h, h)

    def x_copy(c, known):
        arrival = w_recv.at[c] if known is None else p_recv.at[known]
        at = weights.at[c, rows(my_slot)]
        return remote(lead if c == 0 else at, at, x_send, arrival, partner)

    def z_copy(c, j, dist):
        return remote(
            lead if c == 0 else weights.at[c, rows(my_slot)], weights.at[c, rows(my_slot)], z_send.at[j], z_recv.at[heard(d, dist), c],
            device(dist, x),
        )

    def f_copy(c, j, dist):
        at = weights.at[c, rows(slot(dist, x))]
        return remote(at, at, f_send.at[j], w_recv.at[c], partner)

    def e_copy(c, j, dist):
        at = weights.at[c, rows(partner_slot)]
        return remote(at, at, e_send.at[j], w_recv.at[c], device(dist, x))

    def landed(ref, sem):
        remote(ref, ref, x_send, sem, partner).wait_recv()

    def left(ref, sem):
        remote(ref, ref, sem, w_recv.at[0], partner).wait_send()

    def from_peer(c, dist):
        landed(weights.at[c, rows(slot(dist, x))], z_recv.at[heard(dist, d), c])

    def from_partner(c, known):
        landed(weights.at[c, rows(partner_slot)], p_recv.at[known])

    def rest(c, known):
        count = h - 1 if known else h
        landed(weights.at[c, pl.ds(0, count * depth)], w_recv.at[c])

    def own_wait():
        at = weights.at[:, rows(my_slot)]
        pltpu.make_async_copy(at, at, hs_sem.at[3]).wait()

    def send_gain(peers):
        remote(gain, gains.at[my_slot], g_sem, g_recv.at[h - 1], partner).start()
        for dist, _ in peers:
            remote(
                gain, gains.at[my_slot], g_sem, g_recv.at[heard(d, dist)], device(dist, x)
            ).start()

    def pass_gain(peers):
        for dist, _ in peers:
            at = gains.at[slot(dist, x)]
            landed(at, g_recv.at[heard(dist, d)])
            remote(at, at, g_sem, g_recv.at[h - 1], partner).start()

    a_copy = remote(hs_v.at[:, away], a_in.at[d], a_sem.at[0], a_sem.at[1 + d], other_half(0))

    @pl.when(is_inner)
    def _():
        send_gain(inner_peers)
        hs_copy.wait()
        a_copy.start()
        lead_copy.wait()
        for c in range(chunks):
            if c == 1:
                own_wait()
            if c < 2:
                x_copy(c, c if c < early else None).start()
            for j, (dist, _) in enumerate(inner_peers):
                z_copy(c, j, dist).start()

    @pl.when(jnp.logical_not(is_inner))
    def _():
        send_gain(outer_peers)
        lead_copy.wait()
        for c in range(first):
            if c == 1:
                own_wait()
            for j, (dist, _) in enumerate(outer_peers):
                z_copy(c, j, dist).start()
        for c in list(range(split, chunks)) + list(range(early)):
            x_copy(c, c - split if c >= split else None).start()

    gain_copy = pltpu.make_async_copy(gain, gains.at[my_slot], g_recv.at[h - 1])
    gain_copy.start()
    home_copy.start()
    for j in range(1, replicas):
        columns = pl.ds(pl.multiple_of(replica_at(j) * own_w, own_w), own_w)
        remote(
            deltas.at[:, columns], d_in.at[j - 1], d_sem.at[0], d_sem.at[1],
            {"replica": replica_at(j)},
        ).start()
    for copy in loads:
        copy.start()

    @pl.when(is_inner)
    def _():
        pass_gain(inner_peers)

    @pl.when(jnp.logical_not(is_inner))
    def _():
        pass_gain(outer_peers)
        hs_copy.wait()
        a_copy.start()
        for c in range(first, chunks):
            for j, (dist, _) in enumerate(outer_peers):
                z_copy(c, j, dist).start()

    home_copy.wait()
    total = jnp.zeros((tokens, 1), jnp.float32)
    part_w = 2 * depth
    for k in range(features // part_w):
        part = hs_v[:, k * part_w : (k + 1) * part_w].astype(jnp.float32)
        total += jnp.sum(part * part, axis=1, keepdims=True)
    inv[...] = jnp.broadcast_to(lax.rsqrt(total / features + 1e-05), inv.shape)

    def scale(target, origin, base):
        for q in range(2 * h):
            at = pl.ds(base + q * depth, depth)
            target[:, q * depth : (q + 1) * depth] = (
                origin[:, at].astype(jnp.float32) * gains[q].astype(jnp.float32)
            ).astype(jnp.bfloat16)

    def scale_own():
        landed(gains.at[pl.ds(0, h + 1)], g_recv.at[h - 1])

        @pl.when(half == 0)
        def _():
            scale(a_own, hs_v, 0)

        @pl.when(half == 1)
        def _():
            scale(a_own, hs_v, half_depth)

    def own_product(c):
        acc[c] = jnp.dot(a_own[...], weights[c], preferred_element_type=jnp.float32)

    def away_product(i, c, final=False):
        c_out[i, c] = jnp.dot(
            a_scaled[i], weights[c], preferred_element_type=jnp.float32
        ).astype(jnp.bfloat16)
        remote(
            c_out.at[i, c], c_in.at[c], c_send, c_recv.at[1 if final else 0], other_half(i)
        ).start()

    def outer_step():
        pltpu.make_async_copy(state, state, load_sem.at[0]).wait()
        landed(d_in, d_sem.at[1])
        avg = deltas_own[...]
        for j in range(1, replicas):
            avg += d_in[j - 1]
        avg = avg / replicas
        moved = 0.9 * momentum[...] + avg
        momentum_new[...] = moved
        outer_new[...] = outer[...] - 0.7 * (avg + 0.9 * moved)
        for j in range(1, replicas):
            remote(
                outer_new, o_in.at[j - 1], o_sem.at[0], o_sem.at[1], {"replica": replica_at(j)}
            ).start()

    def merge_step():
        part = jnp.float32(0.5)
        loads[-1].wait()
        local_new[:, mine] = (
            part * local[:, mine].astype(jnp.float32) + part * outer_new[...]
        ).astype(jnp.bfloat16)
        landed(o_in, o_sem.at[1])
        for j in range(1, replicas):
            theirs = pl.ds(
                pl.multiple_of(lax.rem(r + replicas - j, replicas) * own_w, own_w), own_w
            )
            local_new[:, theirs] = (
                part * local[:, theirs].astype(jnp.float32) + part * o_in[j - 1]
            ).astype(jnp.bfloat16)

    @pl.when(is_inner)
    def _():
        def pass_on(c):
            for j, (dist, _) in enumerate(inner_peers):
                from_peer(c, dist)
                if c < split:
                    f_copy(c, j, dist).start()

        def take(i):
            landed(a_in.at[i], a_sem.at[1 + i])
            for q in range(2 * h):
                at = slice(q * depth, (q + 1) * depth)
                a_scaled[i, :, at] = (
                    a_in[i, :, at].astype(jnp.float32) * gains[q].astype(jnp.float32)
                ).astype(jnp.bfloat16)

        for c in range(first):
            pass_on(c)
            if c + 2 <= first:
                x_copy(c + 2, None).start()
            if c < early:
                from_partner(c, c)
                for j, (dist, _) in enumerate(inner_peers):
                    e_copy(c, j, dist).start()
            if c == 0:
                outer_step()
            if c == 1:
                merge_step()
        for c in range(first + 1, split):
            x_copy(c, None).start()

        scale_own()

        @pl.loop(0, early)
        def _(c):
            rest(c, True)
            own_product(c)

        @pl.loop(early, first)
        def _(c):
            rest(c, False)
            own_product(c)

        for i in reversed(range(h)):
            take(i)

            @pl.loop(0, first)
            def _(c):
                away_product(i, c)

        pass_on(first)
        for c in range(first, chunks):
            if c + 1 < chunks:
                pass_on(c + 1)
            if c + 1 == split - 1:
                for k in range(split, chunks):
                    x_copy(k, None).start()
            rest(c, False)
            for i in reversed(range(h)):
                away_product(i, c, c == chunks - 1)
            own_product(c)

    @pl.when(jnp.logical_not(is_inner))
    def _():
        for c in range(chunks):
            for j, (dist, _) in enumerate(outer_peers):
                from_peer(c, dist)
                if c >= early:
                    f_copy(c, j, dist).start()
            if early <= c < split:
                x_copy(c, None).start()
            if c == 1:
                outer_step()
            if c == 2:
                merge_step()

        scale_own()

        def finish(c, known):
            rest(c, known)
            own_product(c)

        @pl.loop(0, early)
        def _(c):
            finish(c, False)

        for k in range(split, chunks):
            from_partner(k, k - split)
            for j, (dist, inner) in enumerate(outer_peers):
                if inner:
                    e_copy(k, j, dist).start()

        @pl.loop(early, split)
        def _(c):
            finish(c, False)

        @pl.loop(split, chunks)
        def _(c):
            finish(c, True)

    landed(rotation, load_sem.at[1])

    def summed(c):
        return (acc[c] + c_in[c].astype(jnp.float32)) * inv[:, 0:1]

    landed(c_in.at[pl.ds(0, chunks - 1)], c_recv.at[0])

    @pl.loop(0, per_weight)
    def _(c):
        value = summed(c)
        for k in range(width // HEAD):
            head = value[:, k * HEAD : (k + 1) * HEAD]
            turned = head * cosine[...] + pltpu.roll(head, HEAD // 2, 1) * sine[...]
            at = pl.ds(pl.multiple_of(c * width + k * HEAD, HEAD), HEAD)
            keys[:, at] = turned.astype(jnp.bfloat16)

    @pl.loop(0, per_weight - 1)
    def _(c):
        at = pl.ds(pl.multiple_of(c * width, width), width)
        values[:, at] = summed(c + per_weight).astype(jnp.bfloat16)

    a_copy.wait_send()
    left(d_in, d_sem.at[0])
    left(o_in, o_sem.at[0])
    left(gains.at[pl.ds(0, 2 * h - 1)], g_sem)
    left(weights.at[:, rows(my_slot)], x_send)
    for j in range(h - 1):
        left(weights.at[:, rows(my_slot)], z_send.at[j])
        left(weights.at[pl.ds(0, split), rows(my_slot)], f_send.at[j])

    @pl.when(is_inner)
    def _():
        for j in range(h - 1):
            left(weights.at[pl.ds(0, early), rows(my_slot)], e_send.at[j])

    @pl.when(jnp.logical_not(is_inner))
    def _():
        left(weights.at[pl.ds(0, early), rows(my_slot)], e_send.at[0])

    landed(c_in.at[chunks - 1], c_recv.at[1])
    values[:, pl.ds((per_weight - 1) * width, width)] = summed(chunks - 1).astype(jnp.bfloat16)

    @pl.when(is_inner)
    def _():
        left(c_out, c_send)


def per_device(
    groups, replicas,
    hidden_states, norm_gain, key_weight, value_weight, deltas, outer_params, momentum, local_params,
):
    hs, kw, vw = hidden_states[0], key_weight[0], value_weight[0]
    tokens, features = hs.shape
    depth, kv = kw.shape
    width = 2 * HEAD
    chunks = 2 * kv // width
    h = groups // 2
    half_depth = groups * depth
    cosine, sine = rotation_tables(tokens, HEAD)
    own = outer_params.shape
    vmem = pl.BlockSpec(memory_space=pltpu.VMEM)
    hbm = pl.BlockSpec(memory_space=pl.ANY)
    dma = pltpu.SemaphoreType.DMA
    bf16, f32 = jnp.bfloat16, jnp.float32
    results = pl.pallas_call(
        functools.partial(kernel, groups, replicas, width),
        out_shape=(
            pltpu.VMEM((tokens, kv), bf16),
            pltpu.VMEM((tokens, kv), bf16),
            pltpu.VMEM(own, f32),
            pltpu.VMEM(own, f32),
            pltpu.VMEM(local_params.shape[1:], bf16),
        ),
        in_specs=[hbm] * 10,
        out_specs=[vmem] * 5,
        scratch_shapes=[
            pltpu.VMEM((2, tokens, HEAD), f32),
            pltpu.VMEM((3,) + own, f32),
            pltpu.VMEM(local_params.shape[1:], bf16),
            pltpu.VMEM((depth, width), bf16),
            pltpu.VMEM((tokens, features), bf16),
            pltpu.VMEM((2 * h, 1, depth), bf16),
            pltpu.VMEM((h, tokens, half_depth), bf16),
            pltpu.VMEM((h, tokens, half_depth), bf16),
            pltpu.VMEM((tokens, half_depth), bf16),
            pltpu.VMEM((chunks, half_depth, width), bf16),
            pltpu.VMEM((tokens, HEAD), f32),
            pltpu.VMEM((chunks, tokens, width), f32),
            pltpu.VMEM((h, chunks, tokens, width), bf16),
            pltpu.VMEM((chunks, tokens, width), bf16),
            pltpu.VMEM((replicas - 1,) + own, f32),
            pltpu.VMEM((replicas - 1,) + own, f32),
            dma((4,)),
            dma,
            dma((h,)),
            dma((1 + h,)),
            dma((h - 1, chunks)),
            dma((chunks // 4,)),
            dma((chunks,)),
            dma,
            dma((h - 1,)),
            dma((h - 1,)),
            dma((h - 1,)),
            dma,
            dma((2,)),
            dma((2,)),
            dma((2,)),
            dma((3,)),
        ],
        compiler_params=pltpu.CompilerParams(
            collective_id=0, has_side_effects=True, vmem_limit_bytes=60 * 1024 * 1024
        ),
    )(
        hs, norm_gain, kw, vw, cosine, sine,
        deltas[0], outer_params, momentum, local_params[0],
    )
    keys, values, momentum_new, outer_new, local_new = pl.pallas_call(
        write_out,
        out_shape=tuple(jax.ShapeDtypeStruct(a.shape, a.dtype) for a in results),
        in_specs=[vmem] * 5,
        out_specs=[hbm] * 5,
        scratch_shapes=[dma((5,))],
        compiler_params=pltpu.CompilerParams(vmem_limit_bytes=1024 * 1024),
    )(*results)
    return keys[None], values[None], momentum_new, outer_new, local_new[None]


def solution(mesh):
    in_specs = (
        P("replica", "fsdp", None),
        P("replica", "fsdp"),
        P("replica", "fsdp", None),
        P("replica", "fsdp", None),
        P("replica", "fsdp", None),
        P("fsdp", "replica"),
        P("fsdp", "replica"),
        P("replica", "fsdp", None),
    )
    out_specs = (
        P("replica", "fsdp", None),
        P("replica", "fsdp", None),
        P("fsdp", "replica"),
        P("fsdp", "replica"),
        P("replica", "fsdp", None),
    )
    groups, replicas = mesh.shape["fsdp"] // 2, mesh.shape["replica"]
    return jax.shard_map(
        functools.partial(per_device, groups, replicas),
        mesh=mesh, in_specs=in_specs, out_specs=out_specs, check_vma=False,
    )
```

```python
import functools

import jax
import jax.numpy as jnp
import numpy as np
from jax import lax
from jax.experimental import pallas as pl
from jax.experimental.pallas import tpu as pltpu
from jax.sharding import PartitionSpec as P

HEAD = 128
MESH = pl.DeviceIdType.MESH


def rotation_tables(tokens, head_size):
    half_width = head_size // 2
    exponent = np.arange(half_width, dtype=np.float32) * np.float32(2.0 / head_size)
    frequency = np.power(np.float32(500000.0), -exponent)
    angles = np.arange(tokens, dtype=np.float32)[:, None] * frequency[None, :]
    cosine, sine = np.cos(angles), np.sin(angles)
    return (
        jnp.asarray(np.concatenate([cosine, cosine], axis=1)),
        jnp.asarray(np.concatenate([-sine, sine], axis=1)),
    )


def write_out(*refs):
    count = len(refs) // 2
    sems = refs[-1]
    copies = [
        pltpu.make_async_copy(refs[i], refs[count + i], sems.at[i]) for i in range(count)
    ]
    for copy in copies:
        copy.start()
    for copy in copies:
        copy.wait()


def kernel(
    groups, replicas, width,
    hs, gain, kw, vw, cosine_in, sine_in, deltas, outer_in, momentum_in, local_in,
    keys, values, momentum_new, outer_new, local_new,
    rotation, state, local, lead,
    hs_v, gains, a_in, a_scaled, a_own, weights, inv, acc, c_out, c_in, d_in, o_in,
    hs_sem, g_sem, g_recv, a_sem, z_recv, p_recv, w_recv, x_send, z_send, f_send, e_send,
    c_send, c_recv, d_sem, o_sem, load_sem,
):
    h = groups // 2
    r, f = lax.axis_index("replica"), lax.axis_index("fsdp")
    x, g = lax.rem(f, 2), lax.div(f, 2)
    half = lax.div(g, h)
    local_g = lax.rem(g, h)
    d = (h - 1 - local_g) * (1 - half) + local_g * half
    tokens, depth = hs.shape[0], kw.shape[0]
    half_depth = 2 * h * depth
    per_weight = kw.shape[1] // width
    chunks = 2 * per_weight
    first = chunks // 2 - 1
    split = chunks - chunks // 4
    early = chunks // 4
    own_w = outer_in.shape[1]
    cosine, sine = rotation.at[0], rotation.at[1]
    deltas_own, outer, momentum = state.at[0], state.at[1], state.at[2]
    features = hs.shape[1]

    def place(dist):
        return (h - 1 - dist) * (1 - half) + dist * half

    def slot(dist, side):
        return 2 * place(dist) + side

    def device(dist, side):
        return {"fsdp": 2 * (half * h + place(dist)) + side}

    def other_half(dist):
        return {"fsdp": 2 * ((1 - half) * (h + dist) + half * (h - 1 - dist)) + x}

    partner = device(d, 1 - x)
    outer_peers = [(0, True)] + [(1 + lax.rem(d - 1 + j, h - 1), False) for j in range(1, h - 1)]
    inner_peers = [(j, False) for j in range(1, h)]
    is_inner = d == 0
    late = lax.rem(r, 2) == 0

    def replica_at(j):
        return lax.rem(r + j, replicas)

    barrier = pltpu.get_barrier_semaphore()

    def greet(target):
        pl.semaphore_signal(barrier, inc=1, device_id=target, device_id_type=MESH)

    greet(partner)
    for j in range(1, replicas):
        greet({"replica": replica_at(j)})

    @pl.when(is_inner)
    def _():
        greet(other_half(0))
        for dist, _ in inner_peers:
            greet(device(dist, x))

    @pl.when(jnp.logical_not(is_inner))
    def _():
        for dist, _ in outer_peers:
            greet(device(dist, x))

    def remote(src, dst, send, recv, target):
        return pltpu.make_async_remote_copy(
            src_ref=src, dst_ref=dst, send_sem=send, recv_sem=recv,
            device_id=target, device_id_type=MESH,
        )

    mine = pl.ds(pl.multiple_of(r * own_w, own_w), own_w)
    away = pl.ds(pl.multiple_of((1 - half) * half_depth, half_depth), half_depth)
    home = pl.ds(pl.multiple_of(half * half_depth, half_depth), half_depth)
    hs_copy = pltpu.make_async_copy(hs.at[:, away], hs_v.at[:, away], hs_sem.at[0])
    hs_copy.start()
    lead_copy = pltpu.make_async_copy(kw.at[:, pl.ds(0, width)], lead, hs_sem.at[2])
    lead_copy.start()
    home_copy = pltpu.make_async_copy(hs.at[:, home], hs_v.at[:, home], hs_sem.at[1])
    my_slot = slot(d, x)
    partner_slot = slot(d, 1 - x)

    def rows(q):
        return pl.ds(pl.multiple_of(q * depth, depth), depth)

    def source(c):
        return (kw if c < per_weight else vw).at[:, pl.ds((c % per_weight) * width, width)]

    own_copies = [
        pltpu.make_async_copy(source(c), weights.at[c, rows(my_slot)], hs_sem.at[3])
        for c in range(chunks)
    ]
    loads = [
        pltpu.make_async_copy(src, dst, load_sem.at[i])
        for i, src, dst in (
            (0, deltas.at[:, mine], deltas_own),
            (0, outer_in, outer),
            (0, momentum_in, momentum),
            (1, cosine_in, cosine),
            (1, sine_in, sine),
            (2, local_in, local),
        )
    ]

    for copy in own_copies:
        copy.start()
    pl.semaphore_wait(barrier, 1 + (h - 1) + (replicas - 1) + jnp.where(is_inner, 1, 0))

    def heard(sender, receiver):
        return lax.rem(sender - receiver - 1 + h, h)

    def x_copy(c, known):
        arrival = w_recv.at[c] if known is None else p_recv.at[known]
        at = weights.at[c, rows(my_slot)]
        return remote(lead if c == 0 else at, at, x_send, arrival, partner)

    def z_copy(c, j, dist):
        return remote(
            lead if c == 0 else weights.at[c, rows(my_slot)], weights.at[c, rows(my_slot)], z_send.at[j], z_recv.at[heard(d, dist), c],
            device(dist, x),
        )

    def f_copy(c, j, dist):
        at = weights.at[c, rows(slot(dist, x))]
        return remote(at, at, f_send.at[j], w_recv.at[c], partner)

    def e_copy(c, j, dist):
        at = weights.at[c, rows(partner_slot)]
        return remote(at, at, e_send.at[j], w_recv.at[c], device(dist, x))

    def landed(ref, sem):
        remote(ref, ref, x_send, sem, partner).wait_recv()

    def left(ref, sem):
        remote(ref, ref, sem, w_recv.at[0], partner).wait_send()

    def from_peer(c, dist):
        landed(weights.at[c, rows(slot(dist, x))], z_recv.at[heard(dist, d), c])

    def from_partner(c, known):
        landed(weights.at[c, rows(partner_slot)], p_recv.at[known])

    def rest(c, known):
        count = h - 1 if known else h
        landed(weights.at[c, pl.ds(0, count * depth)], w_recv.at[c])

    def own_wait():
        at = weights.at[:, rows(my_slot)]
        pltpu.make_async_copy(at, at, hs_sem.at[3]).wait()

    def send_gain(peers):
        remote(gain, gains.at[my_slot], g_sem, g_recv.at[h - 1], partner).start()
        for dist, _ in peers:
            remote(
                gain, gains.at[my_slot], g_sem, g_recv.at[heard(d, dist)], device(dist, x)
            ).start()

    def pass_gain(peers):
        for dist, _ in peers:
            at = gains.at[slot(dist, x)]
            landed(at, g_recv.at[heard(dist, d)])
            remote(at, at, g_sem, g_recv.at[h - 1], partner).start()

    a_copy = remote(hs_v.at[:, away], a_in.at[d], a_sem.at[0], a_sem.at[1 + d], other_half(0))

    @pl.when(is_inner)
    def _():
        send_gain(inner_peers)
        hs_copy.wait()
        a_copy.start()
        lead_copy.wait()
        for c in range(chunks):
            if c == 1:
                own_wait()
            if c < 2:
                x_copy(c, c if c < early else None).start()
            for j, (dist, _) in enumerate(inner_peers):
                z_copy(c, j, dist).start()

    @pl.when(jnp.logical_not(is_inner))
    def _():
        send_gain(outer_peers)
        lead_copy.wait()
        for c in range(first):
            if c == 1:
                own_wait()
            for j, (dist, _) in enumerate(outer_peers):
                z_copy(c, j, dist).start()
        for c in list(range(split, chunks)) + list(range(early)):
            x_copy(c, c - split if c >= split else None).start()

    gain_copy = pltpu.make_async_copy(gain, gains.at[my_slot], g_recv.at[h - 1])
    gain_copy.start()
    home_copy.start()
    for j in range(1, replicas):
        columns = pl.ds(pl.multiple_of(replica_at(j) * own_w, own_w), own_w)
        remote(
            deltas.at[:, columns], d_in.at[j - 1], d_sem.at[0], d_sem.at[1],
            {"replica": replica_at(j)},
        ).start()
    for copy in loads:
        copy.start()

    @pl.when(is_inner)
    def _():
        pass_gain(inner_peers)

    @pl.when(jnp.logical_not(is_inner))
    def _():
        pass_gain(outer_peers)
        hs_copy.wait()
        a_copy.start()
        for c in range(first, chunks):
            for j, (dist, _) in enumerate(outer_peers):
                z_copy(c, j, dist).start()

    home_copy.wait()
    total = jnp.zeros((tokens, 1), jnp.float32)
    part_w = 2 * depth
    for k in range(features // part_w):
        part = hs_v[:, k * part_w : (k + 1) * part_w].astype(jnp.float32)
        total += jnp.sum(part * part, axis=1, keepdims=True)
    inv[...] = jnp.broadcast_to(lax.rsqrt(total / features + 1e-05), inv.shape)

    def scale(target, origin, base):
        for q in range(2 * h):
            at = pl.ds(base + q * depth, depth)
            target[:, q * depth : (q + 1) * depth] = (
                origin[:, at].astype(jnp.float32) * gains[q].astype(jnp.float32)
            ).astype(jnp.bfloat16)

    def scale_own():
        landed(gains.at[pl.ds(0, h + 1)], g_recv.at[h - 1])

        @pl.when(half == 0)
        def _():
            scale(a_own, hs_v, 0)

        @pl.when(half == 1)
        def _():
            scale(a_own, hs_v, half_depth)

    def own_product(c):
        acc[c] = jnp.dot(a_own[...], weights[c], preferred_element_type=jnp.float32)

    def away_send(i, c, final=False):
        remote(
            c_out.at[i, c], c_in.at[c], c_send, c_recv.at[1 if final else 0], other_half(i)
        ).start()

    def away_product(i, c):
        c_out[i, c] = jnp.dot(
            a_scaled[i], weights[c], preferred_element_type=jnp.float32
        ).astype(jnp.bfloat16)

    def outer_step():
        pltpu.make_async_copy(state, state, load_sem.at[0]).wait()
        landed(d_in, d_sem.at[1])
        avg = deltas_own[...]
        for j in range(1, replicas):
            avg += d_in[j - 1]
        avg = avg / replicas
        moved = 0.9 * momentum[...] + avg
        momentum_new[...] = moved
        outer_new[...] = outer[...] - 0.7 * (avg + 0.9 * moved)
        for j in range(1, replicas):
            remote(
                outer_new, o_in.at[j - 1], o_sem.at[0], o_sem.at[1], {"replica": replica_at(j)}
            ).start()

    def merge_step():
        part = jnp.float32(0.5)
        loads[-1].wait()
        local_new[:, mine] = (
            part * local[:, mine].astype(jnp.float32) + part * outer_new[...]
        ).astype(jnp.bfloat16)
        landed(o_in, o_sem.at[1])
        for j in range(1, replicas):
            theirs = pl.ds(
                pl.multiple_of(lax.rem(r + replicas - j, replicas) * own_w, own_w), own_w
            )
            local_new[:, theirs] = (
                part * local[:, theirs].astype(jnp.float32) + part * o_in[j - 1]
            ).astype(jnp.bfloat16)

    @pl.when(is_inner)
    def _():
        def pass_on(c):
            for j, (dist, _) in enumerate(inner_peers):
                from_peer(c, dist)
                if c < split:
                    f_copy(c, j, dist).start()

        def take(i):
            landed(a_in.at[i], a_sem.at[1 + i])
            for q in range(2 * h):
                at = slice(q * depth, (q + 1) * depth)
                a_scaled[i, :, at] = (
                    a_in[i, :, at].astype(jnp.float32) * gains[q].astype(jnp.float32)
                ).astype(jnp.bfloat16)

        for c in range(first):
            pass_on(c)
            if c + 2 <= first:
                x_copy(c + 2, None).start()
            if c < early:
                from_partner(c, c)
                for j, (dist, _) in enumerate(inner_peers):
                    e_copy(c, j, dist).start()
            if c == 0:
                outer_step()
            if c == 1:
                merge_step()
        for c in range(first + 1, split):
            x_copy(c, None).start()

        scale_own()

        @pl.loop(0, early)
        def _(c):
            rest(c, True)
            own_product(c)

        @pl.loop(early, first)
        def _(c):
            rest(c, False)
            own_product(c)

        for i in reversed(range(h)):
            take(i)

            @pl.loop(0, first)
            def _(c):
                away_product(i, c)
                away_send(i, c)

        pass_on(first)
        for c in range(first, chunks):
            if c + 1 < chunks:
                pass_on(c + 1)
            if c + 1 == split - 1:
                for k in range(split, chunks):
                    x_copy(k, None).start()
            rest(c, False)
            for i in reversed(range(h)):
                away_product(i, c)
                if i == 0 and c == chunks - 1:
                    pl.when(late)(functools.partial(away_send, i, c - 1))
                if i > 0 or c != chunks - 2:
                    away_send(i, c, c == chunks - 1)
                else:
                    pl.when(jnp.logical_not(late))(functools.partial(away_send, i, c))
            own_product(c)

    @pl.when(jnp.logical_not(is_inner))
    def _():
        for c in range(chunks):
            for j, (dist, _) in enumerate(outer_peers):
                from_peer(c, dist)
                if c >= early:
                    f_copy(c, j, dist).start()
            if early <= c < split:
                x_copy(c, None).start()
            if c == 1:
                outer_step()
            if c == 2:
                merge_step()

        scale_own()

        def finish(c, known):
            rest(c, known)
            own_product(c)

        @pl.loop(0, early)
        def _(c):
            finish(c, False)

        for k in range(split, chunks):
            from_partner(k, k - split)
            for j, (dist, inner) in enumerate(outer_peers):
                if inner:
                    e_copy(k, j, dist).start()

        @pl.loop(early, split)
        def _(c):
            finish(c, False)

        @pl.loop(split, chunks)
        def _(c):
            finish(c, True)

    landed(rotation, load_sem.at[1])

    def summed(c):
        return (acc[c] + c_in[c].astype(jnp.float32)) * inv[:, 0:1]

    landed(c_in.at[pl.ds(0, chunks - 1)], c_recv.at[0])

    @pl.loop(0, per_weight)
    def _(c):
        value = summed(c)
        for k in range(width // HEAD):
            head = value[:, k * HEAD : (k + 1) * HEAD]
            turned = head * cosine[...] + pltpu.roll(head, HEAD // 2, 1) * sine[...]
            at = pl.ds(pl.multiple_of(c * width + k * HEAD, HEAD), HEAD)
            keys[:, at] = turned.astype(jnp.bfloat16)

    @pl.loop(0, per_weight - 1)
    def _(c):
        at = pl.ds(pl.multiple_of(c * width, width), width)
        values[:, at] = summed(c + per_weight).astype(jnp.bfloat16)

    a_copy.wait_send()
    left(d_in, d_sem.at[0])
    left(o_in, o_sem.at[0])
    left(gains.at[pl.ds(0, 2 * h - 1)], g_sem)
    left(weights.at[:, rows(my_slot)], x_send)
    for j in range(h - 1):
        left(weights.at[:, rows(my_slot)], z_send.at[j])
        left(weights.at[pl.ds(0, split), rows(my_slot)], f_send.at[j])

    @pl.when(is_inner)
    def _():
        for j in range(h - 1):
            left(weights.at[pl.ds(0, early), rows(my_slot)], e_send.at[j])

    @pl.when(jnp.logical_not(is_inner))
    def _():
        left(weights.at[pl.ds(0, early), rows(my_slot)], e_send.at[0])

    landed(c_in.at[chunks - 1], c_recv.at[1])
    values[:, pl.ds((per_weight - 1) * width, width)] = summed(chunks - 1).astype(jnp.bfloat16)

    @pl.when(is_inner)
    def _():
        left(c_out, c_send)


def per_device(
    groups, replicas,
    hidden_states, norm_gain, key_weight, value_weight, deltas, outer_params, momentum, local_params,
):
    hs, kw, vw = hidden_states[0], key_weight[0], value_weight[0]
    tokens, features = hs.shape
    depth, kv = kw.shape
    width = 2 * HEAD
    chunks = 2 * kv // width
    h = groups // 2
    half_depth = groups * depth
    cosine, sine = rotation_tables(tokens, HEAD)
    own = outer_params.shape
    vmem = pl.BlockSpec(memory_space=pltpu.VMEM)
    hbm = pl.BlockSpec(memory_space=pl.ANY)
    dma = pltpu.SemaphoreType.DMA
    bf16, f32 = jnp.bfloat16, jnp.float32
    results = pl.pallas_call(
        functools.partial(kernel, groups, replicas, width),
        out_shape=(
            pltpu.VMEM((tokens, kv), bf16),
            pltpu.VMEM((tokens, kv), bf16),
            pltpu.VMEM(own, f32),
            pltpu.VMEM(own, f32),
            pltpu.VMEM(local_params.shape[1:], bf16),
        ),
        in_specs=[hbm] * 10,
        out_specs=[vmem] * 5,
        scratch_shapes=[
            pltpu.VMEM((2, tokens, HEAD), f32),
            pltpu.VMEM((3,) + own, f32),
            pltpu.VMEM(local_params.shape[1:], bf16),
            pltpu.VMEM((depth, width), bf16),
            pltpu.VMEM((tokens, features), bf16),
            pltpu.VMEM((2 * h, 1, depth), bf16),
            pltpu.VMEM((h, tokens, half_depth), bf16),
            pltpu.VMEM((h, tokens, half_depth), bf16),
            pltpu.VMEM((tokens, half_depth), bf16),
            pltpu.VMEM((chunks, half_depth, width), bf16),
            pltpu.VMEM((tokens, HEAD), f32),
            pltpu.VMEM((chunks, tokens, width), f32),
            pltpu.VMEM((h, chunks, tokens, width), bf16),
            pltpu.VMEM((chunks, tokens, width), bf16),
            pltpu.VMEM((replicas - 1,) + own, f32),
            pltpu.VMEM((replicas - 1,) + own, f32),
            dma((4,)),
            dma,
            dma((h,)),
            dma((1 + h,)),
            dma((h - 1, chunks)),
            dma((chunks // 4,)),
            dma((chunks,)),
            dma,
            dma((h - 1,)),
            dma((h - 1,)),
            dma((h - 1,)),
            dma,
            dma((2,)),
            dma((2,)),
            dma((2,)),
            dma((3,)),
        ],
        compiler_params=pltpu.CompilerParams(
            collective_id=0, has_side_effects=True, vmem_limit_bytes=60 * 1024 * 1024
        ),
    )(
        hs, norm_gain, kw, vw, cosine, sine,
        deltas[0], outer_params, momentum, local_params[0],
    )
    keys, values, momentum_new, outer_new, local_new = pl.pallas_call(
        write_out,
        out_shape=tuple(jax.ShapeDtypeStruct(a.shape, a.dtype) for a in results),
        in_specs=[vmem] * 5,
        out_specs=[hbm] * 5,
        scratch_shapes=[dma((5,))],
        compiler_params=pltpu.CompilerParams(vmem_limit_bytes=1024 * 1024),
    )(*results)
    return keys[None], values[None], momentum_new, outer_new, local_new[None]


def solution(mesh):
    in_specs = (
        P("replica", "fsdp", None),
        P("replica", "fsdp"),
        P("replica", "fsdp", None),
        P("replica", "fsdp", None),
        P("replica", "fsdp", None),
        P("fsdp", "replica"),
        P("fsdp", "replica"),
        P("replica", "fsdp", None),
    )
    out_specs = (
        P("replica", "fsdp", None),
        P("replica", "fsdp", None),
        P("fsdp", "replica"),
        P("fsdp", "replica"),
        P("replica", "fsdp", None),
    )
    groups, replicas = mesh.shape["fsdp"] // 2, mesh.shape["replica"]
    return jax.shard_map(
        functools.partial(per_device, groups, replicas),
        mesh=mesh, in_specs=in_specs, out_specs=out_specs, check_vma=False,
    )
```

```python
import functools

import jax
import jax.numpy as jnp
import numpy as np
from jax import lax
from jax.experimental import pallas as pl
from jax.experimental.pallas import tpu as pltpu
from jax.sharding import PartitionSpec as P

HEAD = 128
MESH = pl.DeviceIdType.MESH


def rotation_tables(tokens, head_size):
    half_width = head_size // 2
    exponent = np.arange(half_width, dtype=np.float32) * np.float32(2.0 / head_size)
    frequency = np.power(np.float32(500000.0), -exponent)
    angles = np.arange(tokens, dtype=np.float32)[:, None] * frequency[None, :]
    cosine, sine = np.cos(angles), np.sin(angles)
    return (
        jnp.asarray(np.concatenate([cosine, cosine], axis=1)),
        jnp.asarray(np.concatenate([-sine, sine], axis=1)),
    )


def write_out(*refs):
    count = len(refs) // 2
    sems = refs[-1]
    copies = [
        pltpu.make_async_copy(refs[i], refs[count + i], sems.at[i]) for i in range(count)
    ]
    for copy in copies:
        copy.start()
    for copy in copies:
        copy.wait()


def kernel(
    groups, replicas, width,
    hs, gain, kw, vw, cosine_in, sine_in, deltas, outer_in, momentum_in, local_in,
    keys, values, momentum_new, outer_new, local_new,
    rotation, state, local, lead,
    hs_v, gains, a_in, a_scaled, a_own, weights, inv, acc, c_out, c_in, d_in, o_in,
    hs_sem, g_sem, g_recv, a_sem, z_recv, p_recv, w_recv, x_send, z_send, f_send, e_send,
    c_send, c_recv, d_sem, o_sem, load_sem,
):
    h = groups // 2
    r, f = lax.axis_index("replica"), lax.axis_index("fsdp")
    x, g = lax.rem(f, 2), lax.div(f, 2)
    half = lax.div(g, h)
    local_g = lax.rem(g, h)
    d = (h - 1 - local_g) * (1 - half) + local_g * half
    tokens, depth = hs.shape[0], kw.shape[0]
    half_depth = 2 * h * depth
    per_weight = kw.shape[1] // width
    chunks = 2 * per_weight
    first = chunks // 2 - 1
    split = chunks - chunks // 4
    early = chunks // 4
    own_w = outer_in.shape[1]
    cosine, sine = rotation.at[0], rotation.at[1]
    deltas_own, outer, momentum = state.at[0], state.at[1], state.at[2]
    features = hs.shape[1]

    def place(dist):
        return (h - 1 - dist) * (1 - half) + dist * half

    def slot(dist, side):
        return 2 * place(dist) + side

    def device(dist, side):
        return {"fsdp": 2 * (half * h + place(dist)) + side}

    def other_half(dist):
        return {"fsdp": 2 * ((1 - half) * (h + dist) + half * (h - 1 - dist)) + x}

    partner = device(d, 1 - x)
    outer_peers = [(0, True)] + [(1 + lax.rem(d - 1 + j, h - 1), False) for j in range(1, h - 1)]
    inner_peers = [(j, False) for j in range(1, h)]
    is_inner = d == 0
    late = lax.rem(r, 2) == 0

    def replica_at(j):
        return lax.rem(r + j, replicas)

    barrier = pltpu.get_barrier_semaphore()

    def greet(target):
        pl.semaphore_signal(barrier, inc=1, device_id=target, device_id_type=MESH)

    greet(partner)
    for j in range(1, replicas):
        greet({"replica": replica_at(j)})

    @pl.when(is_inner)
    def _():
        greet(other_half(0))
        for dist, _ in inner_peers:
            greet(device(dist, x))

    @pl.when(jnp.logical_not(is_inner))
    def _():
        for dist, _ in outer_peers:
            greet(device(dist, x))

    def remote(src, dst, send, recv, target):
        return pltpu.make_async_remote_copy(
            src_ref=src, dst_ref=dst, send_sem=send, recv_sem=recv,
            device_id=target, device_id_type=MESH,
        )

    mine = pl.ds(pl.multiple_of(r * own_w, own_w), own_w)
    away = pl.ds(pl.multiple_of((1 - half) * half_depth, half_depth), half_depth)
    home = pl.ds(pl.multiple_of(half * half_depth, half_depth), half_depth)
    hs_copy = pltpu.make_async_copy(hs.at[:, away], hs_v.at[:, away], hs_sem.at[0])
    hs_copy.start()
    lead_copy = pltpu.make_async_copy(kw.at[:, pl.ds(0, width)], lead, hs_sem.at[2])
    lead_copy.start()
    home_copy = pltpu.make_async_copy(hs.at[:, home], hs_v.at[:, home], hs_sem.at[1])
    my_slot = slot(d, x)
    partner_slot = slot(d, 1 - x)

    def rows(q):
        return pl.ds(pl.multiple_of(q * depth, depth), depth)

    def source(c):
        return (kw if c < per_weight else vw).at[:, pl.ds((c % per_weight) * width, width)]

    own_copies = [
        pltpu.make_async_copy(source(c), weights.at[c, rows(my_slot)], hs_sem.at[3])
        for c in range(chunks)
    ]
    loads = [
        pltpu.make_async_copy(src, dst, load_sem.at[i])
        for i, src, dst in (
            (0, deltas.at[:, mine], deltas_own),
            (0, outer_in, outer),
            (0, momentum_in, momentum),
            (1, cosine_in, cosine),
            (1, sine_in, sine),
            (2, local_in, local),
        )
    ]

    for copy in own_copies:
        copy.start()
    pl.semaphore_wait(barrier, 1 + (h - 1) + (replicas - 1) + jnp.where(is_inner, 1, 0))

    def heard(sender, receiver):
        return lax.rem(sender - receiver - 1 + h, h)

    def x_copy(c, known):
        arrival = w_recv.at[c] if known is None else p_recv.at[known]
        at = weights.at[c, rows(my_slot)]
        return remote(lead if c == 0 else at, at, x_send, arrival, partner)

    def z_copy(c, j, dist):
        return remote(
            lead if c == 0 else weights.at[c, rows(my_slot)], weights.at[c, rows(my_slot)], z_send.at[j], z_recv.at[heard(d, dist), c],
            device(dist, x),
        )

    def f_copy(c, j, dist):
        at = weights.at[c, rows(slot(dist, x))]
        return remote(at, at, f_send.at[j], w_recv.at[c], partner)

    def e_copy(c, j, dist):
        at = weights.at[c, rows(partner_slot)]
        return remote(at, at, e_send.at[j], w_recv.at[c], device(dist, x))

    def landed(ref, sem):
        remote(ref, ref, x_send, sem, partner).wait_recv()

    def left(ref, sem):
        remote(ref, ref, sem, w_recv.at[0], partner).wait_send()

    def from_peer(c, dist):
        landed(weights.at[c, rows(slot(dist, x))], z_recv.at[heard(dist, d), c])

    def from_partner(c, known):
        landed(weights.at[c, rows(partner_slot)], p_recv.at[known])

    def rest(c, known):
        count = h - 1 if known else h
        landed(weights.at[c, pl.ds(0, count * depth)], w_recv.at[c])

    def own_wait():
        at = weights.at[:, rows(my_slot)]
        pltpu.make_async_copy(at, at, hs_sem.at[3]).wait()

    def send_gain(peers):
        remote(gain, gains.at[my_slot], g_sem, g_recv.at[h - 1], partner).start()
        for dist, _ in peers:
            remote(
                gain, gains.at[my_slot], g_sem, g_recv.at[heard(d, dist)], device(dist, x)
            ).start()

    def pass_gain(peers):
        for dist, _ in peers:
            at = gains.at[slot(dist, x)]
            landed(at, g_recv.at[heard(dist, d)])
            remote(at, at, g_sem, g_recv.at[h - 1], partner).start()

    a_copy = remote(hs_v.at[:, away], a_in.at[d], a_sem.at[0], a_sem.at[1 + d], other_half(0))

    @pl.when(is_inner)
    def _():
        send_gain(inner_peers)
        hs_copy.wait()
        a_copy.start()
        lead_copy.wait()
        for c in range(chunks):
            if c == 1:
                own_wait()
            if c < 2:
                x_copy(c, c if c < early else None).start()
            for j, (dist, _) in enumerate(inner_peers):
                z_copy(c, j, dist).start()

    @pl.when(jnp.logical_not(is_inner))
    def _():
        send_gain(outer_peers)
        lead_copy.wait()
        for c in range(first):
            if c == 1:
                own_wait()
            for j, (dist, _) in enumerate(outer_peers):
                z_copy(c, j, dist).start()
        for c in list(range(split, chunks)) + list(range(early)):
            x_copy(c, c - split if c >= split else None).start()

    gain_copy = pltpu.make_async_copy(gain, gains.at[my_slot], g_recv.at[h - 1])
    gain_copy.start()
    home_copy.start()
    for j in range(1, replicas):
        columns = pl.ds(pl.multiple_of(replica_at(j) * own_w, own_w), own_w)
        remote(
            deltas.at[:, columns], d_in.at[j - 1], d_sem.at[0], d_sem.at[1],
            {"replica": replica_at(j)},
        ).start()
    for copy in loads:
        copy.start()

    @pl.when(is_inner)
    def _():
        pass_gain(inner_peers)

    @pl.when(jnp.logical_not(is_inner))
    def _():
        pass_gain(outer_peers)
        hs_copy.wait()
        a_copy.start()
        for c in range(first, chunks):
            for j, (dist, _) in enumerate(outer_peers):
                z_copy(c, j, dist).start()

    home_copy.wait()
    total = jnp.zeros((tokens, 1), jnp.float32)
    part_w = 2 * depth
    for k in range(features // part_w):
        part = hs_v[:, k * part_w : (k + 1) * part_w].astype(jnp.float32)
        total += jnp.sum(part * part, axis=1, keepdims=True)
    inv[...] = jnp.broadcast_to(lax.rsqrt(total / features + 1e-05), inv.shape)

    def scale(target, origin, base):
        for q in range(2 * h):
            at = pl.ds(base + q * depth, depth)
            target[:, q * depth : (q + 1) * depth] = (
                origin[:, at].astype(jnp.float32) * gains[q].astype(jnp.float32)
            ).astype(jnp.bfloat16)

    def scale_own():
        landed(gains.at[pl.ds(0, h + 1)], g_recv.at[h - 1])

        @pl.when(half == 0)
        def _():
            scale(a_own, hs_v, 0)

        @pl.when(half == 1)
        def _():
            scale(a_own, hs_v, half_depth)

    def own_product(c):
        acc[c] = jnp.dot(a_own[...], weights[c], preferred_element_type=jnp.float32)

    def away_send(i, c, final=False):
        remote(
            c_out.at[i, c], c_in.at[c], c_send, c_recv.at[1 if final else 0], other_half(i)
        ).start()

    def away_product(i, c):
        c_out[i, c] = jnp.dot(
            a_scaled[i], weights[c], preferred_element_type=jnp.float32
        ).astype(jnp.bfloat16)

    def outer_step():
        pltpu.make_async_copy(state, state, load_sem.at[0]).wait()
        landed(d_in, d_sem.at[1])
        avg = deltas_own[...]
        for j in range(1, replicas):
            avg += d_in[j - 1]
        avg = avg / replicas
        moved = 0.9 * momentum[...] + avg
        momentum_new[...] = moved
        outer_new[...] = outer[...] - 0.7 * (avg + 0.9 * moved)
        for j in range(1, replicas):
            remote(
                outer_new, o_in.at[j - 1], o_sem.at[0], o_sem.at[1], {"replica": replica_at(j)}
            ).start()

    def merge_step():
        part = jnp.float32(0.5)
        loads[-1].wait()
        local_new[:, mine] = (
            part * local[:, mine].astype(jnp.float32) + part * outer_new[...]
        ).astype(jnp.bfloat16)
        landed(o_in, o_sem.at[1])
        for j in range(1, replicas):
            theirs = pl.ds(
                pl.multiple_of(lax.rem(r + replicas - j, replicas) * own_w, own_w), own_w
            )
            local_new[:, theirs] = (
                part * local[:, theirs].astype(jnp.float32) + part * o_in[j - 1]
            ).astype(jnp.bfloat16)

    @pl.when(is_inner)
    def _():
        def pass_on(c):
            for j, (dist, _) in enumerate(inner_peers):
                from_peer(c, dist)
                if c < split:
                    f_copy(c, j, dist).start()

        def take(i):
            landed(a_in.at[i], a_sem.at[1 + i])
            for q in range(2 * h):
                at = slice(q * depth, (q + 1) * depth)
                a_scaled[i, :, at] = (
                    a_in[i, :, at].astype(jnp.float32) * gains[q].astype(jnp.float32)
                ).astype(jnp.bfloat16)

        for c in range(first):
            pass_on(c)
            if c + 2 <= first:
                x_copy(c + 2, None).start()
            if c < early:
                from_partner(c, c)
                for j, (dist, _) in enumerate(inner_peers):
                    e_copy(c, j, dist).start()
            if c == 0:
                outer_step()
            if c == 1:
                merge_step()
        for c in range(first + 1, split):
            x_copy(c, None).start()

        scale_own()

        @pl.loop(0, early)
        def _(c):
            rest(c, True)
            own_product(c)

        @pl.loop(early, first)
        def _(c):
            rest(c, False)
            own_product(c)

        for i in reversed(range(h)):
            take(i)

            @pl.loop(0, first)
            def _(c):
                away_product(i, c)
                away_send(i, c)

        pass_on(first)
        for c in range(first, chunks):
            if c + 1 < chunks:
                pass_on(c + 1)
            if c + 1 == split - 1:
                for k in range(split, chunks):
                    x_copy(k, None).start()
            rest(c, False)
            for i in reversed(range(h)):
                away_product(i, c)
                if i == 0 and c == chunks - 1:
                    pl.when(late)(functools.partial(away_send, i, c - 1))
                if i > 0 or c != chunks - 2:
                    away_send(i, c, c == chunks - 1)
                else:
                    pl.when(jnp.logical_not(late))(functools.partial(away_send, i, c))
            own_product(c)

    @pl.when(jnp.logical_not(is_inner))
    def _():
        for c in range(chunks):
            for j, (dist, inner) in enumerate(outer_peers):
                from_peer(c, dist)
                if c >= early or not inner:
                    f_copy(c, j, dist).start()
            if early <= c < split:
                x_copy(c, None).start()
            if c == 1:
                outer_step()
            if c == 2:
                merge_step()

        scale_own()

        def finish(c, known):
            rest(c, known)
            own_product(c)

        @pl.loop(0, early)
        def _(c):
            finish(c, False)

        for k in range(split, chunks):
            from_partner(k, k - split)
            for j, (dist, inner) in enumerate(outer_peers):
                if inner:
                    e_copy(k, j, dist).start()

        @pl.loop(early, split)
        def _(c):
            finish(c, False)

        @pl.loop(split, chunks)
        def _(c):
            finish(c, True)

    landed(rotation, load_sem.at[1])

    def summed(c):
        return (acc[c] + c_in[c].astype(jnp.float32)) * inv[:, 0:1]

    landed(c_in.at[pl.ds(0, chunks - 1)], c_recv.at[0])

    @pl.loop(0, per_weight)
    def _(c):
        value = summed(c)
        for k in range(width // HEAD):
            head = value[:, k * HEAD : (k + 1) * HEAD]
            turned = head * cosine[...] + pltpu.roll(head, HEAD // 2, 1) * sine[...]
            at = pl.ds(pl.multiple_of(c * width + k * HEAD, HEAD), HEAD)
            keys[:, at] = turned.astype(jnp.bfloat16)

    @pl.loop(0, per_weight - 1)
    def _(c):
        at = pl.ds(pl.multiple_of(c * width, width), width)
        values[:, at] = summed(c + per_weight).astype(jnp.bfloat16)

    a_copy.wait_send()
    left(d_in, d_sem.at[0])
    left(o_in, o_sem.at[0])
    left(gains.at[pl.ds(0, 2 * h - 1)], g_sem)
    left(weights.at[:, rows(my_slot)], x_send)
    for j in range(h - 1):
        left(weights.at[:, rows(my_slot)], z_send.at[j])

    @pl.when(is_inner)
    def _():
        for j in range(h - 1):
            left(weights.at[pl.ds(0, split), rows(my_slot)], f_send.at[j])
            left(weights.at[pl.ds(0, early), rows(my_slot)], e_send.at[j])

    @pl.when(jnp.logical_not(is_inner))
    def _():
        left(weights.at[pl.ds(0, early), rows(my_slot)], e_send.at[0])
        for j, (_, inner) in enumerate(outer_peers):
            passed = split if inner else chunks
            left(weights.at[pl.ds(0, passed), rows(my_slot)], f_send.at[j])

    landed(c_in.at[chunks - 1], c_recv.at[1])
    values[:, pl.ds((per_weight - 1) * width, width)] = summed(chunks - 1).astype(jnp.bfloat16)

    @pl.when(is_inner)
    def _():
        left(c_out, c_send)


def per_device(
    groups, replicas,
    hidden_states, norm_gain, key_weight, value_weight, deltas, outer_params, momentum, local_params,
):
    hs, kw, vw = hidden_states[0], key_weight[0], value_weight[0]
    tokens, features = hs.shape
    depth, kv = kw.shape
    width = 2 * HEAD
    chunks = 2 * kv // width
    h = groups // 2
    half_depth = groups * depth
    cosine, sine = rotation_tables(tokens, HEAD)
    own = outer_params.shape
    vmem = pl.BlockSpec(memory_space=pltpu.VMEM)
    hbm = pl.BlockSpec(memory_space=pl.ANY)
    dma = pltpu.SemaphoreType.DMA
    bf16, f32 = jnp.bfloat16, jnp.float32
    results = pl.pallas_call(
        functools.partial(kernel, groups, replicas, width),
        out_shape=(
            pltpu.VMEM((tokens, kv), bf16),
            pltpu.VMEM((tokens, kv), bf16),
            pltpu.VMEM(own, f32),
            pltpu.VMEM(own, f32),
            pltpu.VMEM(local_params.shape[1:], bf16),
        ),
        in_specs=[hbm] * 10,
        out_specs=[vmem] * 5,
        scratch_shapes=[
            pltpu.VMEM((2, tokens, HEAD), f32),
            pltpu.VMEM((3,) + own, f32),
            pltpu.VMEM(local_params.shape[1:], bf16),
            pltpu.VMEM((depth, width), bf16),
            pltpu.VMEM((tokens, features), bf16),
            pltpu.VMEM((2 * h, 1, depth), bf16),
            pltpu.VMEM((h, tokens, half_depth), bf16),
            pltpu.VMEM((h, tokens, half_depth), bf16),
            pltpu.VMEM((tokens, half_depth), bf16),
            pltpu.VMEM((chunks, half_depth, width), bf16),
            pltpu.VMEM((tokens, HEAD), f32),
            pltpu.VMEM((chunks, tokens, width), f32),
            pltpu.VMEM((h, chunks, tokens, width), bf16),
            pltpu.VMEM((chunks, tokens, width), bf16),
            pltpu.VMEM((replicas - 1,) + own, f32),
            pltpu.VMEM((replicas - 1,) + own, f32),
            dma((4,)),
            dma,
            dma((h,)),
            dma((1 + h,)),
            dma((h - 1, chunks)),
            dma((chunks // 4,)),
            dma((chunks,)),
            dma,
            dma((h - 1,)),
            dma((h - 1,)),
            dma((h - 1,)),
            dma,
            dma((2,)),
            dma((2,)),
            dma((2,)),
            dma((3,)),
        ],
        compiler_params=pltpu.CompilerParams(
            collective_id=0, has_side_effects=True, vmem_limit_bytes=60 * 1024 * 1024
        ),
    )(
        hs, norm_gain, kw, vw, cosine, sine,
        deltas[0], outer_params, momentum, local_params[0],
    )
    keys, values, momentum_new, outer_new, local_new = pl.pallas_call(
        write_out,
        out_shape=tuple(jax.ShapeDtypeStruct(a.shape, a.dtype) for a in results),
        in_specs=[vmem] * 5,
        out_specs=[hbm] * 5,
        scratch_shapes=[dma((5,))],
        compiler_params=pltpu.CompilerParams(vmem_limit_bytes=1024 * 1024),
    )(*results)
    return keys[None], values[None], momentum_new, outer_new, local_new[None]


def solution(mesh):
    in_specs = (
        P("replica", "fsdp", None),
        P("replica", "fsdp"),
        P("replica", "fsdp", None),
        P("replica", "fsdp", None),
        P("replica", "fsdp", None),
        P("fsdp", "replica"),
        P("fsdp", "replica"),
        P("replica", "fsdp", None),
    )
    out_specs = (
        P("replica", "fsdp", None),
        P("replica", "fsdp", None),
        P("fsdp", "replica"),
        P("fsdp", "replica"),
        P("replica", "fsdp", None),
    )
    groups, replicas = mesh.shape["fsdp"] // 2, mesh.shape["replica"]
    return jax.shard_map(
        functools.partial(per_device, groups, replicas),
        mesh=mesh, in_specs=in_specs, out_specs=out_specs, check_vma=False,
    )
```

```python
import functools

import jax
import jax.numpy as jnp
import numpy as np
from jax import lax
from jax.experimental import pallas as pl
from jax.experimental.pallas import tpu as pltpu
from jax.sharding import PartitionSpec as P

HEAD = 128
MESH = pl.DeviceIdType.MESH


def rotation_tables(tokens, head_size):
    half_width = head_size // 2
    exponent = np.arange(half_width, dtype=np.float32) * np.float32(2.0 / head_size)
    frequency = np.power(np.float32(500000.0), -exponent)
    angles = np.arange(tokens, dtype=np.float32)[:, None] * frequency[None, :]
    cosine, sine = np.cos(angles), np.sin(angles)
    return (
        jnp.asarray(np.concatenate([cosine, cosine], axis=1)),
        jnp.asarray(np.concatenate([-sine, sine], axis=1)),
    )


def write_out(*refs):
    count = len(refs) // 2
    sems = refs[-1]
    copies = [
        pltpu.make_async_copy(refs[i], refs[count + i], sems.at[i]) for i in range(count)
    ]
    for copy in copies:
        copy.start()
    for copy in copies:
        copy.wait()


def kernel(
    groups, replicas, width,
    hs, gain, kw, vw, cosine_in, sine_in, deltas, outer_in, momentum_in, local_in,
    keys, values, momentum_new, outer_new, local_new,
    rotation, state, local, lead,
    hs_v, gains, a_in, a_scaled, a_own, weights, inv, acc, c_out, c_in, d_in, o_in,
    hs_sem, g_sem, g_recv, a_sem, z_recv, p_recv, w_recv, x_send, z_send, f_send, e_send,
    c_send, c_recv, d_sem, o_sem, load_sem,
):
    h = groups // 2
    r, f = lax.axis_index("replica"), lax.axis_index("fsdp")
    x, g = lax.rem(f, 2), lax.div(f, 2)
    half = lax.div(g, h)
    local_g = lax.rem(g, h)
    d = (h - 1 - local_g) * (1 - half) + local_g * half
    tokens, depth = hs.shape[0], kw.shape[0]
    half_depth = 2 * h * depth
    per_weight = kw.shape[1] // width
    chunks = 2 * per_weight
    first = chunks // 2 - 1
    split = chunks - chunks // 4
    early = chunks // 4
    own_w = outer_in.shape[1]
    cosine, sine = rotation.at[0], rotation.at[1]
    deltas_own, outer, momentum = state.at[0], state.at[1], state.at[2]
    features = hs.shape[1]

    def place(dist):
        return (h - 1 - dist) * (1 - half) + dist * half

    def slot(dist, side):
        return 2 * place(dist) + side

    def device(dist, side):
        return {"fsdp": 2 * (half * h + place(dist)) + side}

    def other_half(dist):
        return {"fsdp": 2 * ((1 - half) * (h + dist) + half * (h - 1 - dist)) + x}

    partner = device(d, 1 - x)
    outer_peers = [(0, True)] + [(1 + lax.rem(d - 1 + j, h - 1), False) for j in range(1, h - 1)]
    inner_peers = [(j, False) for j in range(1, h)]
    is_inner = d == 0
    late = lax.rem(r, 2) == 0

    def replica_at(j):
        return lax.rem(r + j, replicas)

    barrier = pltpu.get_barrier_semaphore()

    def greet(target):
        pl.semaphore_signal(barrier, inc=1, device_id=target, device_id_type=MESH)

    greet(partner)
    for j in range(1, replicas):
        greet({"replica": replica_at(j)})

    @pl.when(is_inner)
    def _():
        greet(other_half(0))
        for dist, _ in inner_peers:
            greet(device(dist, x))

    @pl.when(jnp.logical_not(is_inner))
    def _():
        for dist, _ in outer_peers:
            greet(device(dist, x))

    def remote(src, dst, send, recv, target):
        return pltpu.make_async_remote_copy(
            src_ref=src, dst_ref=dst, send_sem=send, recv_sem=recv,
            device_id=target, device_id_type=MESH,
        )

    mine = pl.ds(pl.multiple_of(r * own_w, own_w), own_w)
    away = pl.ds(pl.multiple_of((1 - half) * half_depth, half_depth), half_depth)
    home = pl.ds(pl.multiple_of(half * half_depth, half_depth), half_depth)
    hs_copy = pltpu.make_async_copy(hs.at[:, away], hs_v.at[:, away], hs_sem.at[0])
    hs_copy.start()
    lead_copy = pltpu.make_async_copy(kw.at[:, pl.ds(0, width)], lead, hs_sem.at[2])
    lead_copy.start()
    home_copy = pltpu.make_async_copy(hs.at[:, home], hs_v.at[:, home], hs_sem.at[1])
    my_slot = slot(d, x)
    partner_slot = slot(d, 1 - x)

    def rows(q):
        return pl.ds(pl.multiple_of(q * depth, depth), depth)

    def source(c):
        return (kw if c < per_weight else vw).at[:, pl.ds((c % per_weight) * width, width)]

    own_copies = [
        pltpu.make_async_copy(source(c), weights.at[c, rows(my_slot)], hs_sem.at[3])
        for c in range(chunks)
    ]
    loads = [
        pltpu.make_async_copy(src, dst, load_sem.at[i])
        for i, src, dst in (
            (0, deltas.at[:, mine], deltas_own),
            (0, outer_in, outer),
            (0, momentum_in, momentum),
            (1, cosine_in, cosine),
            (1, sine_in, sine),
            (2, local_in, local),
        )
    ]

    for copy in own_copies:
        copy.start()
    pl.semaphore_wait(barrier, 1 + (h - 1) + (replicas - 1) + jnp.where(is_inner, 1, 0))

    def heard(sender, receiver):
        return lax.rem(sender - receiver - 1 + h, h)

    def x_copy(c, known):
        arrival = w_recv.at[c] if known is None else p_recv.at[known]
        at = weights.at[c, rows(my_slot)]
        return remote(lead if c == 0 else at, at, x_send, arrival, partner)

    def z_copy(c, j, dist):
        return remote(
            lead if c == 0 else weights.at[c, rows(my_slot)], weights.at[c, rows(my_slot)], z_send.at[j], z_recv.at[heard(d, dist), c],
            device(dist, x),
        )

    def f_copy(c, j, dist):
        at = weights.at[c, rows(slot(dist, x))]
        return remote(at, at, f_send.at[j], w_recv.at[c], partner)

    def e_copy(c, j, dist):
        at = weights.at[c, rows(partner_slot)]
        return remote(at, at, e_send.at[j], w_recv.at[c], device(dist, x))

    def landed(ref, sem):
        remote(ref, ref, x_send, sem, partner).wait_recv()

    def left(ref, sem):
        remote(ref, ref, sem, w_recv.at[0], partner).wait_send()

    def from_peer(c, dist):
        landed(weights.at[c, rows(slot(dist, x))], z_recv.at[heard(dist, d), c])

    def from_partner(c, known):
        landed(weights.at[c, rows(partner_slot)], p_recv.at[known])

    def rest(c, known):
        count = h - 1 if known else h
        landed(weights.at[c, pl.ds(0, count * depth)], w_recv.at[c])

    def own_wait():
        at = weights.at[:, rows(my_slot)]
        pltpu.make_async_copy(at, at, hs_sem.at[3]).wait()

    def send_gain(peers):
        remote(gain, gains.at[my_slot], g_sem, g_recv.at[h - 1], partner).start()
        for dist, _ in peers:
            remote(
                gain, gains.at[my_slot], g_sem, g_recv.at[heard(d, dist)], device(dist, x)
            ).start()

    def pass_gain(peers):
        for dist, _ in peers:
            at = gains.at[slot(dist, x)]
            landed(at, g_recv.at[heard(dist, d)])
            remote(at, at, g_sem, g_recv.at[h - 1], partner).start()

    a_copy = remote(hs_v.at[:, away], a_in.at[d], a_sem.at[0], a_sem.at[1 + d], other_half(0))

    @pl.when(is_inner)
    def _():
        send_gain(inner_peers)
        hs_copy.wait()
        a_copy.start()
        lead_copy.wait()
        for c in range(chunks):
            if c == 1:
                own_wait()
            if c < 2:
                x_copy(c, c if c < early else None).start()
            for j, (dist, _) in enumerate(inner_peers):
                z_copy(c, j, dist).start()

    @pl.when(jnp.logical_not(is_inner))
    def _():
        send_gain(outer_peers)
        lead_copy.wait()
        for c in range(first):
            if c == 1:
                own_wait()
            for j, (dist, _) in enumerate(outer_peers):
                z_copy(c, j, dist).start()
        for c in list(range(split, chunks)) + list(range(early)):
            x_copy(c, c - split if c >= split else None).start()

    gain_copy = pltpu.make_async_copy(gain, gains.at[my_slot], g_recv.at[h - 1])
    gain_copy.start()
    home_copy.start()
    for j in range(1, replicas):
        columns = pl.ds(pl.multiple_of(replica_at(j) * own_w, own_w), own_w)
        remote(
            deltas.at[:, columns], d_in.at[j - 1], d_sem.at[0], d_sem.at[1],
            {"replica": replica_at(j)},
        ).start()
    for copy in loads:
        copy.start()

    @pl.when(is_inner)
    def _():
        pass_gain(inner_peers)

    @pl.when(jnp.logical_not(is_inner))
    def _():
        pass_gain(outer_peers)
        hs_copy.wait()
        a_copy.start()
        for c in range(first, chunks):
            for j, (dist, _) in enumerate(outer_peers):
                z_copy(c, j, dist).start()

    home_copy.wait()
    total = jnp.zeros((tokens, 1), jnp.float32)
    part_w = 2 * depth
    for k in range(features // part_w):
        part = hs_v[:, k * part_w : (k + 1) * part_w].astype(jnp.float32)
        total += jnp.sum(part * part, axis=1, keepdims=True)
    inv[...] = jnp.broadcast_to(lax.rsqrt(total / features + 1e-05), inv.shape)

    def scale(target, origin, base):
        for q in range(2 * h):
            at = pl.ds(base + q * depth, depth)
            target[:, q * depth : (q + 1) * depth] = (
                origin[:, at].astype(jnp.float32) * gains[q].astype(jnp.float32)
            ).astype(jnp.bfloat16)

    def scale_own():
        landed(gains.at[pl.ds(0, h + 1)], g_recv.at[h - 1])

        @pl.when(half == 0)
        def _():
            scale(a_own, hs_v, 0)

        @pl.when(half == 1)
        def _():
            scale(a_own, hs_v, half_depth)

    def own_product(c):
        acc[c] = jnp.dot(a_own[...], weights[c], preferred_element_type=jnp.float32)

    def away_send(i, c, final=False):
        remote(
            c_out.at[i, c], c_in.at[c], c_send, c_recv.at[1 if final else 0], other_half(i)
        ).start()

    def away_product(i, c):
        c_out[i, c] = jnp.dot(
            a_scaled[i], weights[c], preferred_element_type=jnp.float32
        ).astype(jnp.bfloat16)

    def outer_step():
        pltpu.make_async_copy(state, state, load_sem.at[0]).wait()
        landed(d_in, d_sem.at[1])
        avg = deltas_own[...]
        for j in range(1, replicas):
            avg += d_in[j - 1]
        avg = avg / replicas
        moved = 0.9 * momentum[...] + avg
        momentum_new[...] = moved
        outer_new[...] = outer[...] - 0.7 * (avg + 0.9 * moved)
        for j in range(1, replicas):
            remote(
                outer_new, o_in.at[j - 1], o_sem.at[0], o_sem.at[1], {"replica": replica_at(j)}
            ).start()

    def merge_step():
        part = jnp.float32(0.5)
        loads[-1].wait()
        local_new[:, mine] = (
            part * local[:, mine].astype(jnp.float32) + part * outer_new[...]
        ).astype(jnp.bfloat16)
        landed(o_in, o_sem.at[1])
        for j in range(1, replicas):
            theirs = pl.ds(
                pl.multiple_of(lax.rem(r + replicas - j, replicas) * own_w, own_w), own_w
            )
            local_new[:, theirs] = (
                part * local[:, theirs].astype(jnp.float32) + part * o_in[j - 1]
            ).astype(jnp.bfloat16)

    @pl.when(is_inner)
    def _():
        def pass_on(c):
            for j, (dist, _) in enumerate(inner_peers):
                from_peer(c, dist)
                if c < split:
                    f_copy(c, j, dist).start()

        def take(i):
            landed(a_in.at[i], a_sem.at[1 + i])
            for q in range(2 * h):
                at = slice(q * depth, (q + 1) * depth)
                a_scaled[i, :, at] = (
                    a_in[i, :, at].astype(jnp.float32) * gains[q].astype(jnp.float32)
                ).astype(jnp.bfloat16)

        for c in range(first):
            pass_on(c)
            if c + 2 <= first:
                x_copy(c + 2, None).start()
            if c < early:
                from_partner(c, c)
                for j, (dist, _) in enumerate(inner_peers):
                    e_copy(c, j, dist).start()
            if c == 0:
                outer_step()
            if c == 1:
                merge_step()
        for c in range(first + 1, split):
            x_copy(c, None).start()

        scale_own()

        @pl.loop(0, early)
        def _(c):
            rest(c, True)
            own_product(c)

        @pl.loop(early, first)
        def _(c):
            rest(c, False)
            own_product(c)

        for i in reversed(range(h)):
            take(i)

            @pl.loop(0, first)
            def _(c):
                away_product(i, c)
                away_send(i, c)

        pass_on(first)
        for c in range(first, chunks):
            if c + 1 < chunks:
                pass_on(c + 1)
            if c + 1 == split - 1:
                for k in range(split, chunks):
                    x_copy(k, None).start()
            rest(c, False)
            for i in reversed(range(h)):
                away_product(i, c)
                if c < chunks - 2:
                    away_send(i, c)

            if c >= chunks - 2:
                final = c == chunks - 1

                @pl.when(late)
                def _():
                    for i in range(h - 1, 0, -1):
                        away_send(i, c, final)
                    if final:
                        away_send(0, c - 1)
                        away_send(0, c, True)

                @pl.when(jnp.logical_not(late))
                def _():
                    for i in range(h):
                        away_send(i, c, final)

            own_product(c)

    @pl.when(jnp.logical_not(is_inner))
    def _():
        for c in range(chunks):
            for j, (dist, inner) in enumerate(outer_peers):
                from_peer(c, dist)
                if c >= early or not inner:
                    f_copy(c, j, dist).start()
            if early <= c < split:
                x_copy(c, None).start()
            if c == 1:
                outer_step()
            if c == 2:
                merge_step()

        scale_own()

        def finish(c, known):
            rest(c, known)
            own_product(c)

        @pl.loop(0, early)
        def _(c):
            finish(c, False)

        for k in range(split, chunks):
            from_partner(k, k - split)
            for j, (dist, inner) in enumerate(outer_peers):
                if inner:
                    e_copy(k, j, dist).start()

        @pl.loop(early, split)
        def _(c):
            finish(c, False)

        @pl.loop(split, chunks)
        def _(c):
            finish(c, True)

    landed(rotation, load_sem.at[1])

    def summed(c):
        return (acc[c] + c_in[c].astype(jnp.float32)) * inv[:, 0:1]

    landed(c_in.at[pl.ds(0, chunks - 1)], c_recv.at[0])

    @pl.loop(0, per_weight)
    def _(c):
        value = summed(c)
        for k in range(width // HEAD):
            head = value[:, k * HEAD : (k + 1) * HEAD]
            turned = head * cosine[...] + pltpu.roll(head, HEAD // 2, 1) * sine[...]
            at = pl.ds(pl.multiple_of(c * width + k * HEAD, HEAD), HEAD)
            keys[:, at] = turned.astype(jnp.bfloat16)

    @pl.loop(0, per_weight - 1)
    def _(c):
        at = pl.ds(pl.multiple_of(c * width, width), width)
        values[:, at] = summed(c + per_weight).astype(jnp.bfloat16)

    a_copy.wait_send()
    left(d_in, d_sem.at[0])
    left(o_in, o_sem.at[0])
    left(gains.at[pl.ds(0, 2 * h - 1)], g_sem)
    left(weights.at[:, rows(my_slot)], x_send)
    for j in range(h - 1):
        left(weights.at[:, rows(my_slot)], z_send.at[j])

    @pl.when(is_inner)
    def _():
        for j in range(h - 1):
            left(weights.at[pl.ds(0, split), rows(my_slot)], f_send.at[j])
            left(weights.at[pl.ds(0, early), rows(my_slot)], e_send.at[j])

    @pl.when(jnp.logical_not(is_inner))
    def _():
        left(weights.at[pl.ds(0, early), rows(my_slot)], e_send.at[0])
        for j, (_, inner) in enumerate(outer_peers):
            passed = split if inner else chunks
            left(weights.at[pl.ds(0, passed), rows(my_slot)], f_send.at[j])

    landed(c_in.at[chunks - 1], c_recv.at[1])
    values[:, pl.ds((per_weight - 1) * width, width)] = summed(chunks - 1).astype(jnp.bfloat16)

    @pl.when(is_inner)
    def _():
        left(c_out, c_send)


def per_device(
    groups, replicas,
    hidden_states, norm_gain, key_weight, value_weight, deltas, outer_params, momentum, local_params,
):
    hs, kw, vw = hidden_states[0], key_weight[0], value_weight[0]
    tokens, features = hs.shape
    depth, kv = kw.shape
    width = 2 * HEAD
    chunks = 2 * kv // width
    h = groups // 2
    half_depth = groups * depth
    cosine, sine = rotation_tables(tokens, HEAD)
    own = outer_params.shape
    vmem = pl.BlockSpec(memory_space=pltpu.VMEM)
    hbm = pl.BlockSpec(memory_space=pl.ANY)
    dma = pltpu.SemaphoreType.DMA
    bf16, f32 = jnp.bfloat16, jnp.float32
    results = pl.pallas_call(
        functools.partial(kernel, groups, replicas, width),
        out_shape=(
            pltpu.VMEM((tokens, kv), bf16),
            pltpu.VMEM((tokens, kv), bf16),
            pltpu.VMEM(own, f32),
            pltpu.VMEM(own, f32),
            pltpu.VMEM(local_params.shape[1:], bf16),
        ),
        in_specs=[hbm] * 10,
        out_specs=[vmem] * 5,
        scratch_shapes=[
            pltpu.VMEM((2, tokens, HEAD), f32),
            pltpu.VMEM((3,) + own, f32),
            pltpu.VMEM(local_params.shape[1:], bf16),
            pltpu.VMEM((depth, width), bf16),
            pltpu.VMEM((tokens, features), bf16),
            pltpu.VMEM((2 * h, 1, depth), bf16),
            pltpu.VMEM((h, tokens, half_depth), bf16),
            pltpu.VMEM((h, tokens, half_depth), bf16),
            pltpu.VMEM((tokens, half_depth), bf16),
            pltpu.VMEM((chunks, half_depth, width), bf16),
            pltpu.VMEM((tokens, HEAD), f32),
            pltpu.VMEM((chunks, tokens, width), f32),
            pltpu.VMEM((h, chunks, tokens, width), bf16),
            pltpu.VMEM((chunks, tokens, width), bf16),
            pltpu.VMEM((replicas - 1,) + own, f32),
            pltpu.VMEM((replicas - 1,) + own, f32),
            dma((4,)),
            dma,
            dma((h,)),
            dma((1 + h,)),
            dma((h - 1, chunks)),
            dma((chunks // 4,)),
            dma((chunks,)),
            dma,
            dma((h - 1,)),
            dma((h - 1,)),
            dma((h - 1,)),
            dma,
            dma((2,)),
            dma((2,)),
            dma((2,)),
            dma((3,)),
        ],
        compiler_params=pltpu.CompilerParams(
            collective_id=0, has_side_effects=True, vmem_limit_bytes=60 * 1024 * 1024
        ),
    )(
        hs, norm_gain, kw, vw, cosine, sine,
        deltas[0], outer_params, momentum, local_params[0],
    )
    keys, values, momentum_new, outer_new, local_new = pl.pallas_call(
        write_out,
        out_shape=tuple(jax.ShapeDtypeStruct(a.shape, a.dtype) for a in results),
        in_specs=[vmem] * 5,
        out_specs=[hbm] * 5,
        scratch_shapes=[dma((5,))],
        compiler_params=pltpu.CompilerParams(vmem_limit_bytes=1024 * 1024),
    )(*results)
    return keys[None], values[None], momentum_new, outer_new, local_new[None]


def solution(mesh):
    in_specs = (
        P("replica", "fsdp", None),
        P("replica", "fsdp"),
        P("replica", "fsdp", None),
        P("replica", "fsdp", None),
        P("replica", "fsdp", None),
        P("fsdp", "replica"),
        P("fsdp", "replica"),
        P("replica", "fsdp", None),
    )
    out_specs = (
        P("replica", "fsdp", None),
        P("replica", "fsdp", None),
        P("fsdp", "replica"),
        P("fsdp", "replica"),
        P("replica", "fsdp", None),
    )
    groups, replicas = mesh.shape["fsdp"] // 2, mesh.shape["replica"]
    return jax.shard_map(
        functools.partial(per_device, groups, replicas),
        mesh=mesh, in_specs=in_specs, out_specs=out_specs, check_vma=False,
    )
```

```python
import functools

import jax
import jax.numpy as jnp
import numpy as np
from jax import lax
from jax.experimental import pallas as pl
from jax.experimental.pallas import tpu as pltpu
from jax.sharding import PartitionSpec as P

HEAD = 128
MESH = pl.DeviceIdType.MESH


def rotation_tables(tokens, head_size):
    half_width = head_size // 2
    exponent = np.arange(half_width, dtype=np.float32) * np.float32(2.0 / head_size)
    frequency = np.power(np.float32(500000.0), -exponent)
    angles = np.arange(tokens, dtype=np.float32)[:, None] * frequency[None, :]
    cosine, sine = np.cos(angles), np.sin(angles)
    return (
        jnp.asarray(np.concatenate([cosine, cosine], axis=1)),
        jnp.asarray(np.concatenate([-sine, sine], axis=1)),
    )


def write_out(*refs):
    count = len(refs) // 2
    sems = refs[-1]
    copies = [
        pltpu.make_async_copy(refs[i], refs[count + i], sems.at[i]) for i in range(count)
    ]
    for copy in copies:
        copy.start()
    for copy in copies:
        copy.wait()


def kernel(
    groups, replicas, width,
    hs, gain, kw, vw, cosine_in, sine_in, deltas, outer_in, momentum_in, local_in,
    keys, values, momentum_new, outer_new, local_new,
    rotation, state, local, lead,
    hs_v, gains, a_in, a_scaled, a_own, weights, inv, acc, c_out, c_in, d_in, o_in,
    hs_sem, g_sem, g_recv, a_sem, z_recv, p_recv, w_recv, x_send, z_send, f_send, e_send,
    c_send, c_recv, d_sem, o_sem, load_sem,
):
    h = groups // 2
    r, f = lax.axis_index("replica"), lax.axis_index("fsdp")
    x, g = lax.rem(f, 2), lax.div(f, 2)
    half = lax.div(g, h)
    local_g = lax.rem(g, h)
    d = (h - 1 - local_g) * (1 - half) + local_g * half
    tokens, depth = hs.shape[0], kw.shape[0]
    half_depth = 2 * h * depth
    per_weight = kw.shape[1] // width
    chunks = 2 * per_weight
    first = chunks // 2 - 1
    split = chunks - chunks // 4
    early = chunks // 4
    own_w = outer_in.shape[1]
    cosine, sine = rotation.at[0], rotation.at[1]
    deltas_own, outer, momentum = state.at[0], state.at[1], state.at[2]
    features = hs.shape[1]

    def place(dist):
        return (h - 1 - dist) * (1 - half) + dist * half

    def slot(dist, side):
        return 2 * place(dist) + side

    def device(dist, side):
        return {"fsdp": 2 * (half * h + place(dist)) + side}

    def other_half(dist):
        return {"fsdp": 2 * ((1 - half) * (h + dist) + half * (h - 1 - dist)) + x}

    partner = device(d, 1 - x)
    outer_peers = [(0, True)] + [(1 + lax.rem(d - 1 + j, h - 1), False) for j in range(1, h - 1)]
    inner_peers = [(j, False) for j in range(1, h)]
    is_inner = d == 0
    late = lax.rem(r, 2) == 0

    def replica_at(j):
        return lax.rem(r + j, replicas)

    barrier = pltpu.get_barrier_semaphore()

    def greet(target):
        pl.semaphore_signal(barrier, inc=1, device_id=target, device_id_type=MESH)

    pl.when(is_inner)(functools.partial(greet, other_half(0)))
    greet(partner)
    for j in range(1, replicas):
        greet({"replica": replica_at(j)})

    @pl.when(is_inner)
    def _():
        for dist, _ in inner_peers:
            greet(device(dist, x))

    @pl.when(jnp.logical_not(is_inner))
    def _():
        for dist, _ in outer_peers:
            greet(device(dist, x))

    def remote(src, dst, send, recv, target):
        return pltpu.make_async_remote_copy(
            src_ref=src, dst_ref=dst, send_sem=send, recv_sem=recv,
            device_id=target, device_id_type=MESH,
        )

    mine = pl.ds(pl.multiple_of(r * own_w, own_w), own_w)
    away = pl.ds(pl.multiple_of((1 - half) * half_depth, half_depth), half_depth)
    home = pl.ds(pl.multiple_of(half * half_depth, half_depth), half_depth)
    hs_copy = pltpu.make_async_copy(hs.at[:, away], hs_v.at[:, away], hs_sem.at[0])
    hs_copy.start()
    lead_copy = pltpu.make_async_copy(kw.at[:, pl.ds(0, width)], lead, hs_sem.at[2])
    lead_copy.start()
    home_copy = pltpu.make_async_copy(hs.at[:, home], hs_v.at[:, home], hs_sem.at[1])
    my_slot = slot(d, x)
    partner_slot = slot(d, 1 - x)

    def rows(q):
        return pl.ds(pl.multiple_of(q * depth, depth), depth)

    def source(c):
        return (kw if c < per_weight else vw).at[:, pl.ds((c % per_weight) * width, width)]

    own_copies = [
        pltpu.make_async_copy(source(c), weights.at[c, rows(my_slot)], hs_sem.at[3])
        for c in range(chunks)
    ]
    loads = [
        pltpu.make_async_copy(src, dst, load_sem.at[i])
        for i, src, dst in (
            (0, deltas.at[:, mine], deltas_own),
            (0, outer_in, outer),
            (0, momentum_in, momentum),
            (1, cosine_in, cosine),
            (1, sine_in, sine),
            (2, local_in, local),
        )
    ]

    for copy in own_copies:
        copy.start()
    pl.semaphore_wait(barrier, 1 + (h - 1) + (replicas - 1) + jnp.where(is_inner, 1, 0))

    def heard(sender, receiver):
        return lax.rem(sender - receiver - 1 + h, h)

    def x_copy(c, known):
        arrival = w_recv.at[c] if known is None else p_recv.at[known]
        at = weights.at[c, rows(my_slot)]
        return remote(lead if c == 0 else at, at, x_send, arrival, partner)

    def z_copy(c, j, dist):
        return remote(
            lead if c == 0 else weights.at[c, rows(my_slot)], weights.at[c, rows(my_slot)], z_send.at[j], z_recv.at[heard(d, dist), c],
            device(dist, x),
        )

    def f_copy(c, j, dist):
        at = weights.at[c, rows(slot(dist, x))]
        return remote(at, at, f_send.at[j], w_recv.at[c], partner)

    def e_copy(c, j, dist):
        at = weights.at[c, rows(partner_slot)]
        return remote(at, at, e_send.at[j], w_recv.at[c], device(dist, x))

    def landed(ref, sem):
        remote(ref, ref, x_send, sem, partner).wait_recv()

    def left(ref, sem):
        remote(ref, ref, sem, w_recv.at[0], partner).wait_send()

    def from_peer(c, dist):
        landed(weights.at[c, rows(slot(dist, x))], z_recv.at[heard(dist, d), c])

    def from_partner(c, known):
        landed(weights.at[c, rows(partner_slot)], p_recv.at[known])

    def rest(c, known):
        count = h - 1 if known else h
        landed(weights.at[c, pl.ds(0, count * depth)], w_recv.at[c])

    def own_wait():
        at = weights.at[:, rows(my_slot)]
        pltpu.make_async_copy(at, at, hs_sem.at[3]).wait()

    def send_gain(peers):
        remote(gain, gains.at[my_slot], g_sem, g_recv.at[h - 1], partner).start()
        for dist, _ in peers:
            remote(
                gain, gains.at[my_slot], g_sem, g_recv.at[heard(d, dist)], device(dist, x)
            ).start()

    def pass_gain(peers):
        for dist, _ in peers:
            at = gains.at[slot(dist, x)]
            landed(at, g_recv.at[heard(dist, d)])
            remote(at, at, g_sem, g_recv.at[h - 1], partner).start()

    a_copy = remote(hs_v.at[:, away], a_in.at[d], a_sem.at[0], a_sem.at[1 + d], other_half(0))

    @pl.when(is_inner)
    def _():
        hs_copy.wait()
        a_copy.start()
        send_gain(inner_peers)
        lead_copy.wait()
        for c in range(chunks):
            if c == 1:
                own_wait()
            if c < 2:
                x_copy(c, c if c < early else None).start()
            for j, (dist, _) in enumerate(inner_peers):
                z_copy(c, j, dist).start()

    @pl.when(jnp.logical_not(is_inner))
    def _():
        send_gain(outer_peers)
        lead_copy.wait()
        for c in range(first):
            if c == 1:
                own_wait()
            for j, (dist, _) in enumerate(outer_peers):
                z_copy(c, j, dist).start()
        for c in list(range(split, chunks)) + list(range(early)):
            x_copy(c, c - split if c >= split else None).start()

    gain_copy = pltpu.make_async_copy(gain, gains.at[my_slot], g_recv.at[h - 1])
    gain_copy.start()
    home_copy.start()
    for j in range(1, replicas):
        columns = pl.ds(pl.multiple_of(replica_at(j) * own_w, own_w), own_w)
        remote(
            deltas.at[:, columns], d_in.at[j - 1], d_sem.at[0], d_sem.at[1],
            {"replica": replica_at(j)},
        ).start()
    for copy in loads:
        copy.start()

    @pl.when(is_inner)
    def _():
        pass_gain(inner_peers)

    @pl.when(jnp.logical_not(is_inner))
    def _():
        pass_gain(outer_peers)
        hs_copy.wait()
        a_copy.start()
        for c in range(first, chunks):
            for j, (dist, _) in enumerate(outer_peers):
                z_copy(c, j, dist).start()

    home_copy.wait()
    total = jnp.zeros((tokens, 1), jnp.float32)
    part_w = 2 * depth
    for k in range(features // part_w):
        part = hs_v[:, k * part_w : (k + 1) * part_w].astype(jnp.float32)
        total += jnp.sum(part * part, axis=1, keepdims=True)
    inv[...] = jnp.broadcast_to(lax.rsqrt(total / features + 1e-05), inv.shape)

    def scale(target, origin, base):
        for q in range(2 * h):
            at = pl.ds(base + q * depth, depth)
            target[:, q * depth : (q + 1) * depth] = (
                origin[:, at].astype(jnp.float32) * gains[q].astype(jnp.float32)
            ).astype(jnp.bfloat16)

    def scale_own():
        landed(gains.at[pl.ds(0, h + 1)], g_recv.at[h - 1])

        @pl.when(half == 0)
        def _():
            scale(a_own, hs_v, 0)

        @pl.when(half == 1)
        def _():
            scale(a_own, hs_v, half_depth)

    def own_product(c):
        acc[c] = jnp.dot(a_own[...], weights[c], preferred_element_type=jnp.float32)

    def away_send(i, c, final=False):
        remote(
            c_out.at[i, c], c_in.at[c], c_send, c_recv.at[1 if final else 0], other_half(i)
        ).start()

    def away_product(i, c):
        c_out[i, c] = jnp.dot(
            a_scaled[i], weights[c], preferred_element_type=jnp.float32
        ).astype(jnp.bfloat16)

    def outer_step():
        pltpu.make_async_copy(state, state, load_sem.at[0]).wait()
        landed(d_in, d_sem.at[1])
        avg = deltas_own[...]
        for j in range(1, replicas):
            avg += d_in[j - 1]
        avg = avg / replicas
        moved = 0.9 * momentum[...] + avg
        momentum_new[...] = moved
        outer_new[...] = outer[...] - 0.7 * (avg + 0.9 * moved)
        for j in range(1, replicas):
            remote(
                outer_new, o_in.at[j - 1], o_sem.at[0], o_sem.at[1], {"replica": replica_at(j)}
            ).start()

    def merge_step():
        part = jnp.float32(0.5)
        loads[-1].wait()
        local_new[:, mine] = (
            part * local[:, mine].astype(jnp.float32) + part * outer_new[...]
        ).astype(jnp.bfloat16)
        landed(o_in, o_sem.at[1])
        for j in range(1, replicas):
            theirs = pl.ds(
                pl.multiple_of(lax.rem(r + replicas - j, replicas) * own_w, own_w), own_w
            )
            local_new[:, theirs] = (
                part * local[:, theirs].astype(jnp.float32) + part * o_in[j - 1]
            ).astype(jnp.bfloat16)

    @pl.when(is_inner)
    def _():
        def pass_on(c):
            for j, (dist, _) in enumerate(inner_peers):
                from_peer(c, dist)
                if c < split:
                    f_copy(c, j, dist).start()

        def take(i):
            landed(a_in.at[i], a_sem.at[1 + i])
            for q in range(2 * h):
                at = slice(q * depth, (q + 1) * depth)
                a_scaled[i, :, at] = (
                    a_in[i, :, at].astype(jnp.float32) * gains[q].astype(jnp.float32)
                ).astype(jnp.bfloat16)

        for c in range(first):
            pass_on(c)
            if c + 2 <= first:
                x_copy(c + 2, None).start()
            if c < early:
                from_partner(c, c)
                for j, (dist, _) in enumerate(inner_peers):
                    e_copy(c, j, dist).start()
            if c == 0:
                outer_step()
            if c == 1:
                merge_step()
        for c in range(first + 1, split):
            x_copy(c, None).start()

        scale_own()

        @pl.loop(0, early)
        def _(c):
            rest(c, True)
            own_product(c)

        @pl.loop(early, first)
        def _(c):
            rest(c, False)
            own_product(c)

        for i in reversed(range(h)):
            take(i)

            @pl.loop(0, first)
            def _(c):
                away_product(i, c)
                away_send(i, c)

        pass_on(first)
        for c in range(first, chunks):
            if c + 1 < chunks:
                pass_on(c + 1)
            if c + 1 == split - 1:
                for k in range(split, chunks):
                    x_copy(k, None).start()
            rest(c, False)
            for i in reversed(range(h)):
                away_product(i, c)
                if i == 0 and c == chunks - 1:
                    pl.when(late)(functools.partial(away_send, i, c - 1))
                if i > 0 or c != chunks - 2:
                    away_send(i, c, c == chunks - 1)
                else:
                    pl.when(jnp.logical_not(late))(functools.partial(away_send, i, c))
            own_product(c)

    @pl.when(jnp.logical_not(is_inner))
    def _():
        for c in range(chunks):
            for j, (dist, inner) in enumerate(outer_peers):
                from_peer(c, dist)
                if c >= early or not inner:
                    f_copy(c, j, dist).start()
            if early <= c < split:
                x_copy(c, None).start()
            if c == 1:
                outer_step()
            if c == 2:
                merge_step()

        scale_own()

        def finish(c, known):
            rest(c, known)
            own_product(c)

        @pl.loop(0, early)
        def _(c):
            finish(c, False)

        for k in range(split, chunks):
            from_partner(k, k - split)
            for j, (dist, inner) in enumerate(outer_peers):
                if inner:
                    e_copy(k, j, dist).start()

        @pl.loop(early, split)
        def _(c):
            finish(c, False)

        @pl.loop(split, chunks)
        def _(c):
            finish(c, True)

    landed(rotation, load_sem.at[1])

    def summed(c):
        return (acc[c] + c_in[c].astype(jnp.float32)) * inv[:, 0:1]

    landed(c_in.at[pl.ds(0, chunks - 1)], c_recv.at[0])

    @pl.loop(0, per_weight)
    def _(c):
        value = summed(c)
        for k in range(width // HEAD):
            head = value[:, k * HEAD : (k + 1) * HEAD]
            turned = head * cosine[...] + pltpu.roll(head, HEAD // 2, 1) * sine[...]
            at = pl.ds(pl.multiple_of(c * width + k * HEAD, HEAD), HEAD)
            keys[:, at] = turned.astype(jnp.bfloat16)

    @pl.loop(0, per_weight - 1)
    def _(c):
        at = pl.ds(pl.multiple_of(c * width, width), width)
        values[:, at] = summed(c + per_weight).astype(jnp.bfloat16)

    a_copy.wait_send()
    left(d_in, d_sem.at[0])
    left(o_in, o_sem.at[0])
    left(gains.at[pl.ds(0, 2 * h - 1)], g_sem)
    left(weights.at[:, rows(my_slot)], x_send)
    for j in range(h - 1):
        left(weights.at[:, rows(my_slot)], z_send.at[j])

    @pl.when(is_inner)
    def _():
        for j in range(h - 1):
            left(weights.at[pl.ds(0, split), rows(my_slot)], f_send.at[j])
            left(weights.at[pl.ds(0, early), rows(my_slot)], e_send.at[j])

    @pl.when(jnp.logical_not(is_inner))
    def _():
        left(weights.at[pl.ds(0, early), rows(my_slot)], e_send.at[0])
        for j, (_, inner) in enumerate(outer_peers):
            passed = split if inner else chunks
            left(weights.at[pl.ds(0, passed), rows(my_slot)], f_send.at[j])

    landed(c_in.at[chunks - 1], c_recv.at[1])
    values[:, pl.ds((per_weight - 1) * width, width)] = summed(chunks - 1).astype(jnp.bfloat16)

    @pl.when(is_inner)
    def _():
        left(c_out, c_send)


def per_device(
    groups, replicas,
    hidden_states, norm_gain, key_weight, value_weight, deltas, outer_params, momentum, local_params,
):
    hs, kw, vw = hidden_states[0], key_weight[0], value_weight[0]
    tokens, features = hs.shape
    depth, kv = kw.shape
    width = 2 * HEAD
    chunks = 2 * kv // width
    h = groups // 2
    half_depth = groups * depth
    cosine, sine = rotation_tables(tokens, HEAD)
    own = outer_params.shape
    vmem = pl.BlockSpec(memory_space=pltpu.VMEM)
    hbm = pl.BlockSpec(memory_space=pl.ANY)
    dma = pltpu.SemaphoreType.DMA
    bf16, f32 = jnp.bfloat16, jnp.float32
    results = pl.pallas_call(
        functools.partial(kernel, groups, replicas, width),
        out_shape=(
            pltpu.VMEM((tokens, kv), bf16),
            pltpu.VMEM((tokens, kv), bf16),
            pltpu.VMEM(own, f32),
            pltpu.VMEM(own, f32),
            pltpu.VMEM(local_params.shape[1:], bf16),
        ),
        in_specs=[hbm] * 10,
        out_specs=[vmem] * 5,
        scratch_shapes=[
            pltpu.VMEM((2, tokens, HEAD), f32),
            pltpu.VMEM((3,) + own, f32),
            pltpu.VMEM(local_params.shape[1:], bf16),
            pltpu.VMEM((depth, width), bf16),
            pltpu.VMEM((tokens, features), bf16),
            pltpu.VMEM((2 * h, 1, depth), bf16),
            pltpu.VMEM((h, tokens, half_depth), bf16),
            pltpu.VMEM((h, tokens, half_depth), bf16),
            pltpu.VMEM((tokens, half_depth), bf16),
            pltpu.VMEM((chunks, half_depth, width), bf16),
            pltpu.VMEM((tokens, HEAD), f32),
            pltpu.VMEM((chunks, tokens, width), f32),
            pltpu.VMEM((h, chunks, tokens, width), bf16),
            pltpu.VMEM((chunks, tokens, width), bf16),
            pltpu.VMEM((replicas - 1,) + own, f32),
            pltpu.VMEM((replicas - 1,) + own, f32),
            dma((4,)),
            dma,
            dma((h,)),
            dma((1 + h,)),
            dma((h - 1, chunks)),
            dma((chunks // 4,)),
            dma((chunks,)),
            dma,
            dma((h - 1,)),
            dma((h - 1,)),
            dma((h - 1,)),
            dma,
            dma((2,)),
            dma((2,)),
            dma((2,)),
            dma((3,)),
        ],
        compiler_params=pltpu.CompilerParams(
            collective_id=0, has_side_effects=True, vmem_limit_bytes=60 * 1024 * 1024
        ),
    )(
        hs, norm_gain, kw, vw, cosine, sine,
        deltas[0], outer_params, momentum, local_params[0],
    )
    keys, values, momentum_new, outer_new, local_new = pl.pallas_call(
        write_out,
        out_shape=tuple(jax.ShapeDtypeStruct(a.shape, a.dtype) for a in results),
        in_specs=[vmem] * 5,
        out_specs=[hbm] * 5,
        scratch_shapes=[dma((5,))],
        compiler_params=pltpu.CompilerParams(vmem_limit_bytes=1024 * 1024),
    )(*results)
    return keys[None], values[None], momentum_new, outer_new, local_new[None]


def solution(mesh):
    in_specs = (
        P("replica", "fsdp", None),
        P("replica", "fsdp"),
        P("replica", "fsdp", None),
        P("replica", "fsdp", None),
        P("replica", "fsdp", None),
        P("fsdp", "replica"),
        P("fsdp", "replica"),
        P("replica", "fsdp", None),
    )
    out_specs = (
        P("replica", "fsdp", None),
        P("replica", "fsdp", None),
        P("fsdp", "replica"),
        P("fsdp", "replica"),
        P("replica", "fsdp", None),
    )
    groups, replicas = mesh.shape["fsdp"] // 2, mesh.shape["replica"]
    return jax.shard_map(
        functools.partial(per_device, groups, replicas),
        mesh=mesh, in_specs=in_specs, out_specs=out_specs, check_vma=False,
    )
```
